8 devices in a mesh: dp: 2 (over z, y), cp: 4 (over x, core).
Axes of the slice: x: 2, y: 2, z: 1, core: 2. Of those that a mesh axis runs over, the one named last changes fastest.
Arguments:
- hidden_states: bfloat16 [32, 128, 2048], P('dp', 'cp')
- norm_gain: float32 [2048], replicated
- w_gate: bfloat16 [2048, 11008], replicated
- w_up: bfloat16 [2048, 11008], replicated
- w_down: bfloat16 [11008, 2048], replicated
- final_gain: float32 [2048], replicated
- w_value: float32 [2048], replicated
- b_value: float32 [], replicated
- rewards: float32 [32, 128], P('dp', 'cp')
- mask: int32 [32, 128], P('dp', 'cp')
Outputs:
- output 1: float32 [32, 128], P('dp', 'cp')
- output 2: float32 [32, 128], P('dp', 'cp')
- output 3: float32 [32, 128], P('dp', 'cp')
All inputs are finite; a program needn't handle non-finite values.
Results may differ from the reference program's by a relative error of at most 0.001.
Values sent between devices are 32-bit elements.
A program may use at most 1 GiB of HBM per device.

```python
import jax
import jax.numpy as jnp
from jax import lax

ROW_COUNT = 32
SEQ_LEN = 128
MODEL_DIM = 2048
FFN_DIM = 11008
NORM_EPS = 1e-6
WHITEN_EPS = 1e-8
DISCOUNT = 1.0
GAE_LAMBDA = 0.995


def draw_mask(start_key, end_key):
    starts = jax.random.randint(start_key, (ROW_COUNT,), 0, SEQ_LEN // 2)
    ends = starts + jax.random.randint(end_key, (ROW_COUNT,), 0, SEQ_LEN - starts)
    positions = jnp.arange(SEQ_LEN)[None, :]
    inside = (positions >= starts[:, None]) & (positions <= ends[:, None])
    return inside.astype(jnp.int32), ends


def setup_inputs(seed: int = 0) -> dict:
    keys = jax.random.split(jax.random.key(seed), 12)
    hidden_states = jax.random.normal(keys[0], (ROW_COUNT, SEQ_LEN, MODEL_DIM), jnp.float32).astype(jnp.bfloat16)
    norm_gain = 1.0 + 0.3 * jax.random.normal(keys[1], (MODEL_DIM,), jnp.float32)
    w_gate = (jax.random.normal(keys[2], (MODEL_DIM, FFN_DIM), jnp.float32) * MODEL_DIM ** -0.5).astype(jnp.bfloat16)
    w_up = (jax.random.normal(keys[3], (MODEL_DIM, FFN_DIM), jnp.float32) * MODEL_DIM ** -0.5).astype(jnp.bfloat16)
    w_down = (jax.random.normal(keys[4], (FFN_DIM, MODEL_DIM), jnp.float32) * FFN_DIM ** -0.5).astype(jnp.bfloat16)
    final_gain = 1.0 + 0.3 * jax.random.normal(keys[5], (MODEL_DIM,), jnp.float32)
    w_value = jax.random.normal(keys[6], (MODEL_DIM,), jnp.float32) * MODEL_DIM ** -0.5
    b_value = jax.random.uniform(keys[7], (), jnp.float32, 0.5, 1.0)
    mask, ends = draw_mask(keys[8], keys[9])
    shaping = 0.05 * jax.random.normal(keys[10], (ROW_COUNT, SEQ_LEN), jnp.float32)
    score = 2.0 * jax.random.normal(keys[11], (ROW_COUNT,), jnp.float32)
    at_end = jnp.arange(SEQ_LEN)[None, :] == ends[:, None]
    rewards = shaping + jnp.where(at_end, score[:, None], 0.0)
    return dict(hidden_states=hidden_states, norm_gain=norm_gain, w_gate=w_gate, w_up=w_up, w_down=w_down, final_gain=final_gain, w_value=w_value, b_value=b_value, rewards=rewards, mask=mask)


def reference(hidden_states, norm_gain, w_gate, w_up, w_down, final_gain, w_value, b_value, rewards, mask):
    head_vec = final_gain * w_value

    def row_value(x_row):
        x_f32 = x_row.astype(jnp.float32)
        normed = (x_f32 * lax.rsqrt(jnp.mean(x_f32 * x_f32, axis=-1, keepdims=True) + NORM_EPS) * norm_gain).astype(jnp.bfloat16)
        gate = jnp.dot(normed, w_gate, preferred_element_type=jnp.float32)
        up_val = jnp.dot(normed, w_up, preferred_element_type=jnp.float32)
        hidden = (jax.nn.silu(gate) * up_val).astype(jnp.bfloat16)
        resid = x_f32 + jnp.dot(hidden, w_down, preferred_element_type=jnp.float32)
        resid_n = resid * lax.rsqrt(jnp.mean(resid * resid, axis=-1, keepdims=True) + NORM_EPS)
        return jnp.sum(resid_n * head_vec, axis=-1) + b_value

    mask_f = mask.astype(jnp.float32)
    values = mask_f * lax.map(row_value, hidden_states)
    rew_masked = mask_f * rewards
    next_vals = jnp.concatenate([values[:, 1:], jnp.zeros_like(values[:, :1])], axis=1)
    delta = rew_masked + DISCOUNT * next_vals - values

    def back_step(carry, delta_col):
        adv_col = delta_col + DISCOUNT * GAE_LAMBDA * carry
        return adv_col, adv_col

    _, adv_cols = lax.scan(back_step, jnp.zeros_like(delta[:, 0]), delta.T, reverse=True)
    advantage = adv_cols.T
    count = jnp.sum(mask_f)
    mean_adv = jnp.sum(mask_f * advantage) / count
    var_adv = jnp.sum(mask_f * advantage * advantage) / count - mean_adv * mean_adv
    white = mask_f * (advantage - mean_adv) * lax.rsqrt(var_adv + WHITEN_EPS)
    return values, mask_f * (advantage + values), white
```

```python
import functools
import math

import jax
import jax.numpy as jnp
from jax import lax
from jax.experimental import pallas as pl
from jax.experimental.pallas import tpu as pltpu
from jax.sharding import PartitionSpec as P

NORM_EPS = 1e-6
WHITEN_EPS = 1e-8
DISCOUNT = 1.0
GAE_LAMBDA = 0.995
MESH = pl.DeviceIdType.MESH

ROWS, PIECE, CP, DP = 16, 32, 4, 2
SEQ = PIECE * CP
TOK = ROWS * PIECE
HALF = TOK // 2
SEND_CHUNKS = 4
FC = 256
SLOTS = 8
VARIANTS = (192, 224, 256, 288, 320, 384, 448, 512)


def iota(shape, dim):
    return lax.broadcasted_iota(jnp.int32, shape, dim)


def everyone(dp, cp):
    for step in range(1, DP * CP):
        yield lax.rem(dp + step // CP, DP), lax.rem(cp + step % CP, CP)


def token_row(placed):
    spread = (lax.rem(iota((SEQ, TOK), 0), PIECE) == lax.rem(iota((SEQ, TOK), 1), PIECE)).astype(jnp.bfloat16)
    by_row = jnp.dot(placed.astype(jnp.bfloat16), spread, preferred_element_type=jnp.float32)
    own = iota((ROWS, TOK), 0) == iota((ROWS, TOK), 1) // PIECE
    return jnp.sum(jnp.where(own, by_row, 0.0), axis=0, keepdims=True)


def token_rank(row):
    upper = (iota((TOK, TOK), 0) <= iota((TOK, TOK), 1)).astype(jnp.bfloat16)
    upto = jnp.dot(jnp.broadcast_to(row, (8, TOK)).astype(jnp.bfloat16), upper, preferred_element_type=jnp.float32)[:1]
    return jnp.where(row > 0.0, upto - 1.0, -1.0)


def gather_kernel(x_hbm, mask_ref, rew_ref, xs_ref, tid_ref, cnt_ref, gm_ref,
                  x_v, sendbuf, recvbuf, pack, packs, place, x_sem, pk_send, pk_recv, x_send, x_recv):
    dp, cp = lax.axis_index('dp'), lax.axis_index('cp')
    mate = cp + 1 - 2 * lax.rem(cp, 2)
    load = pltpu.make_async_copy(x_hbm, x_v, x_sem)
    load.start()
    barrier = pltpu.get_barrier_semaphore()
    for to in everyone(dp, cp):
        pl.semaphore_signal(barrier, inc=1, device_id=to, device_id_type=MESH)

    mask_f = mask_ref[...].astype(jnp.float32)
    for half, block in enumerate((mask_f, jnp.where(mask_f > 0.0, rew_ref[...], 0.0))):
        place[half] = jnp.zeros((ROWS, SEQ), jnp.float32)
        place[half, :, :PIECE] = block
        base = place[half]
        moved = base
        for piece in range(1, CP):
            moved = jnp.where(cp == piece, pltpu.roll(base, piece * PIECE, 1), moved)
        pack[half] = moved
    row = token_row(pack[0])
    rank = token_rank(row)
    pl.semaphore_wait(barrier, DP * CP - 1)

    me = dp * CP + cp
    shares = []
    for k, to in enumerate(everyone(dp, cp)):
        share = pltpu.make_async_remote_copy(
            src_ref=pack, dst_ref=packs.at[k], send_sem=pk_send.at[k], recv_sem=pk_recv.at[k],
            device_id=to, device_id_type=MESH)
        share.start()
        shares.append(share)

    load.wait()
    send_rank = (2 * iota((HALF, TOK), 0) + 1).astype(jnp.float32)
    pick = (rank == send_rank).astype(jnp.bfloat16)
    width = x_v.shape[1] // SEND_CHUNKS
    moves = []
    for j in range(SEND_CHUNKS):
        cols = slice(j * width, (j + 1) * width)
        sendbuf[j] = jnp.dot(pick, x_v[:, cols], preferred_element_type=jnp.float32)
        move = pltpu.make_async_remote_copy(
            src_ref=sendbuf.at[j], dst_ref=recvbuf.at[j], send_sem=x_send.at[j], recv_sem=x_recv.at[j],
            device_id=(dp, mate), device_id_type=MESH)
        move.start()
        moves.append(move)

    for share in shares:
        share.wait_recv()
    placed = [[pack[half] for half in range(2)]] + [[packs[k, half] for half in range(2)] for k in range(DP * CP - 1)]
    same = [sum(placed[k][half] for k in range(CP)) for half in range(2)]
    other = [sum(placed[k][half] for k in range(CP, 2 * CP)) for half in range(2)]
    for half in range(2):
        gm_ref[half, :ROWS, :] = same[half]
        gm_ref[half, ROWS:, :] = other[half]
    lane = iota((ROWS, SEQ), 1)
    mate_row = token_row(jnp.where(lane // PIECE == mate, same[0], 0.0))
    mate_rank = token_rank(mate_row)
    got = jnp.floor(jnp.sum(mate_row, axis=1, keepdims=True) * 0.5)
    keep = jnp.floor((jnp.sum(row, axis=1, keepdims=True) + 1.0) * 0.5)
    cnt_ref[...] = jnp.broadcast_to(got + keep, (8, 128))

    slot = iota((TOK, TOK), 0).astype(jnp.float32)
    own = rank == 2.0 * (slot - got)
    own = jnp.logical_and(own, slot >= got)
    tok = iota((1, TOK), 1)
    code = ((tok // PIECE) * SEQ + lax.rem(tok, PIECE)).astype(jnp.float32)
    own_code = code + (cp * PIECE).astype(jnp.float32)
    mate_code = code + (mate * PIECE).astype(jnp.float32)
    theirs = mate_rank == send_rank
    tid = jnp.sum(jnp.where(own, own_code, 0.0), axis=1, keepdims=True)
    tid_ref[...] = tid.astype(jnp.int32)
    tid_ref[:HALF, :] = (tid[:HALF] + jnp.sum(jnp.where(theirs, mate_code, 0.0), axis=1, keepdims=True)).astype(jnp.int32)
    own_pick = own.astype(jnp.bfloat16)
    came = iota((HALF, width), 0).astype(jnp.float32) < got
    for j in range(SEND_CHUNKS):
        cols = slice(j * width, (j + 1) * width)
        xs_ref[:, cols] = jnp.dot(own_pick, x_v[:, cols], preferred_element_type=jnp.float32).astype(jnp.bfloat16)
    for j in range(SEND_CHUNKS):
        cols = slice(j * width, (j + 1) * width)
        moves[j].wait_recv()
        xs_ref[:HALF, cols] = jnp.where(came, recvbuf[j], xs_ref[:HALF, cols].astype(jnp.float32)).astype(jnp.bfloat16)
    for share in shares:
        share.wait_send()
    for move in moves:
        move.wait_send()


def mlp_kernel(cnt_ref, xs_ref, tid_ref, gain_ref, head_ref, bv_ref, wg_hbm, wu_hbm, wd_hbm, out_ref,
               wg_buf, wu_buf, wd_buf, xn, acc, inner, col, sems):
    model = xs_ref.shape[1]
    chunks = wd_hbm.shape[0] // FC

    def copies(i, which=(0, 1, 2)):
        slot = lax.rem(i, SLOTS)
        at = pl.ds(pl.multiple_of(i * FC, FC), FC)
        make = (lambda: pltpu.make_async_copy(wg_hbm.at[:, at], wg_buf.at[slot], sems.at[0, slot]),
                lambda: pltpu.make_async_copy(wu_hbm.at[:, at], wu_buf.at[slot], sems.at[1, slot]),
                lambda: pltpu.make_async_copy(wd_hbm.at[at, :], wd_buf.at[slot], sems.at[2, slot]))
        return [make[w]() for w in which]

    def wait(i):
        for copy in copies(i):
            copy.wait()

    def refill(i):
        @pl.when(i + SLOTS < chunks)
        def _():
            for copy in copies(i + SLOTS):
                copy.start()

    for i in range(SLOTS):
        for copy in copies(jnp.int32(i)):
            copy.start()
    count = jnp.max(cnt_ref[...]).astype(jnp.int32)

    blocks = (count + 31) // 32

    def norm(b, _):
        rows = pl.ds(pl.multiple_of(b * 32, 32), 32)
        x = xs_ref[rows, :].astype(jnp.float32)
        scale = lax.rsqrt(jnp.mean(x * x, axis=-1, keepdims=True) + NORM_EPS)
        xn[rows, :] = (x * scale * gain_ref[...]).astype(jnp.bfloat16)
        return 0

    lax.fori_loop(0, blocks, norm, 0)

    def run(size):
        def inside(i, where):
            slot = lax.rem(i, SLOTS)
            gate = jnp.dot(xn[:size, :], wg_buf[slot], preferred_element_type=jnp.float32)
            up = jnp.dot(xn[:size, :], wu_buf[slot], preferred_element_type=jnp.float32)
            inner[:size, where * FC:(where + 1) * FC] = (jax.nn.silu(gate) * up).astype(jnp.bfloat16)

        def down(i, where):
            return jnp.dot(inner[:size, where * FC:(where + 1) * FC], wd_buf[lax.rem(i, SLOTS)],
                           preferred_element_type=jnp.float32)

        wait(jnp.int32(0))
        inside(jnp.int32(0), 0)
        acc[:size, :] = down(jnp.int32(0), 0)

        def body(j, _):
            first, second = 2 * j + 1, 2 * j + 2
            wait(first)
            wait(second)
            refill(first - 1)
            @pl.when(j > 0)
            def _():
                refill(first - 2)
            inside(first, 0)
            inside(second, 1)
            acc[:size, :] += down(first, 0) + down(second, 1)
            return 0

        lax.fori_loop(0, (chunks - 1) // 2, body, 0)

    for k, size in enumerate(VARIANTS):
        above = VARIANTS[k - 1] if k else -1
        @pl.when(jnp.logical_and(count > above, count <= size))
        def _():
            run(size)

    col[...] = jnp.zeros_like(col)

    def head(b, _):
        rows = pl.ds(pl.multiple_of(b * 32, 32), 32)
        h = xs_ref[rows, :].astype(jnp.float32) + acc[rows, :]
        scale = lax.rsqrt(jnp.mean(h * h, axis=-1, keepdims=True) + NORM_EPS)
        val = jnp.sum(h * head_ref[...], axis=-1, keepdims=True) * scale + bv_ref[0]
        val = jnp.where(iota((32, 1), 0) + b * 32 < count, val, 0.0)
        col[rows, :] = jnp.broadcast_to(val, (32, SEQ))
        return 0

    lax.fori_loop(0, blocks, head, 0)
    at_row = (tid_ref[...] // SEQ == iota((TOK, ROWS), 1)).astype(jnp.float32)
    at_lane = jnp.where(lax.rem(tid_ref[...], SEQ) == iota((TOK, SEQ), 1), col[...], 0.0)
    out_ref[...] = lax.dot_general(at_row, at_lane, (((0,), (0,)), ((), ())), precision=lax.Precision.HIGHEST,
                                   preferred_element_type=jnp.float32)


def gae_kernel(vals_ref, gm_ref, v_ref, ret_ref, white_ref, came, send, recv):
    dp, cp = lax.axis_index('dp'), lax.axis_index('cp')
    barrier = pltpu.get_barrier_semaphore()
    for to in everyone(dp, cp):
        pl.semaphore_signal(barrier, inc=1, device_id=to, device_id_type=MESH)
    pl.semaphore_wait(barrier, DP * CP - 1)
    shares = []
    for k, to in enumerate(everyone(dp, cp)):
        share = pltpu.make_async_remote_copy(
            src_ref=vals_ref, dst_ref=came.at[k], send_sem=send.at[k], recv_sem=recv.at[k],
            device_id=to, device_id_type=MESH)
        share.start()
        shares.append(share)
    for share in shares:
        share.wait_recv()
    same = vals_ref[...] + came[0] + came[1] + came[2]
    other = came[3] + came[4] + came[5] + came[6]
    values = jnp.concatenate([same, other], axis=0)
    mask, rew = gm_ref[0], gm_ref[1]
    lane = iota((2 * ROWS, SEQ), 1)

    def ahead(z, step):
        return jnp.where(lane < SEQ - step, pltpu.roll(z, SEQ - step, 1), 0.0)

    adv = rew + DISCOUNT * ahead(values, 1) - values
    step = 1
    while step < SEQ:
        adv = adv + math.pow(DISCOUNT * GAE_LAMBDA, step) * ahead(adv, step)
        step *= 2

    def total(z):
        return jnp.sum(jnp.sum(z, axis=0, keepdims=True), axis=1, keepdims=True)

    count = total(mask)
    mean = total(mask * adv) / count
    var = total(mask * adv * adv) / count - mean * mean
    white = mask * (adv - mean) * lax.rsqrt(var + WHITEN_EPS)
    for out, z in ((v_ref, values), (ret_ref, mask * (adv + values)), (white_ref, white)):
        mine = z[:ROWS]
        moved = mine
        for piece in range(1, CP):
            moved = jnp.where(cp == piece, pltpu.roll(mine, SEQ - piece * PIECE, 1), moved)
        out[...] = moved[:, :PIECE]
    for share in shares:
        share.wait_send()


def vmem():
    return pl.BlockSpec(memory_space=pltpu.VMEM)


def smem():
    return pl.BlockSpec(memory_space=pltpu.SMEM)


def hbm():
    return pl.BlockSpec(memory_space=pl.ANY)


def solution(mesh):
    def local_step(x_blk, norm_gain, w_gate, w_up, w_down, final_gain, w_value, b_value, rew_blk, mask_blk):
        rows, piece, model = x_blk.shape
        f32, bf16 = jnp.float32, jnp.bfloat16
        x = x_blk.reshape(TOK, model)
        width = model // SEND_CHUNKS
        xs, tid, cnt, gm = pl.pallas_call(
            gather_kernel,
            name='gather_tokens',
            out_shape=(jax.ShapeDtypeStruct((TOK, model), bf16), jax.ShapeDtypeStruct((TOK, 1), jnp.int32),
                       jax.ShapeDtypeStruct((8, 128), f32), jax.ShapeDtypeStruct((2, DP * ROWS, SEQ), f32)),
            in_specs=[hbm(), vmem(), vmem()],
            out_specs=(vmem(),) * 4,
            scratch_shapes=[
                pltpu.VMEM((TOK, model), bf16),
                pltpu.VMEM((SEND_CHUNKS, HALF, width), f32), pltpu.VMEM((SEND_CHUNKS, HALF, width), f32),
                pltpu.VMEM((2, ROWS, SEQ), f32), pltpu.VMEM((DP * CP - 1, 2, ROWS, SEQ), f32),
                pltpu.VMEM((2, ROWS, SEQ), f32),
                pltpu.SemaphoreType.DMA,
                pltpu.SemaphoreType.DMA((DP * CP - 1,)), pltpu.SemaphoreType.DMA((DP * CP - 1,)),
                pltpu.SemaphoreType.DMA((SEND_CHUNKS,)), pltpu.SemaphoreType.DMA((SEND_CHUNKS,)),
            ],
            compiler_params=pltpu.CompilerParams(collective_id=0, has_side_effects=True, vmem_limit_bytes=40 << 20),
        )(x, mask_blk, rew_blk)
        vals = pl.pallas_call(
            mlp_kernel,
            name='active_mlp',
            out_shape=jax.ShapeDtypeStruct((ROWS, SEQ), f32),
            in_specs=[vmem(), vmem(), vmem(), vmem(), vmem(), smem(), hbm(), hbm(), hbm()],
            out_specs=vmem(),
            scratch_shapes=[
                pltpu.VMEM((SLOTS, model, FC), bf16), pltpu.VMEM((SLOTS, model, FC), bf16),
                pltpu.VMEM((SLOTS, FC, model), bf16),
                pltpu.VMEM((TOK, model), bf16), pltpu.VMEM((TOK, model), f32), pltpu.VMEM((TOK, 2 * FC), bf16),
                pltpu.VMEM((TOK, SEQ), f32),
                pltpu.SemaphoreType.DMA((3, SLOTS)),
            ],
            compiler_params=pltpu.CompilerParams(vmem_limit_bytes=60 << 20),
        )(cnt, xs, tid, norm_gain.reshape(1, model), (final_gain * w_value).reshape(1, model), b_value.reshape(1),
          w_gate, w_up, w_down)
        block = jax.ShapeDtypeStruct((rows, piece), f32)
        return pl.pallas_call(
            gae_kernel,
            name='gae',
            out_shape=(block, block, block),
            in_specs=[vmem(), vmem()],
            out_specs=(vmem(),) * 3,
            scratch_shapes=[
                pltpu.VMEM((DP * CP - 1, ROWS, SEQ), f32),
                pltpu.SemaphoreType.DMA((DP * CP - 1,)), pltpu.SemaphoreType.DMA((DP * CP - 1,)),
            ],
            compiler_params=pltpu.CompilerParams(collective_id=1, has_side_effects=True),
        )(vals, gm)

    tok_spec = P('dp', 'cp')
    in_specs = (P('dp', 'cp', None), P(None), P(None, None), P(None, None), P(None, None), P(None), P(None), P(),
                tok_spec, tok_spec)
    return jax.shard_map(local_step, mesh=mesh, in_specs=in_specs, out_specs=(tok_spec,) * 3, check_vma=False)
```

```python
import functools
import math

import jax
import jax.numpy as jnp
from jax import lax
from jax.experimental import pallas as pl
from jax.experimental.pallas import tpu as pltpu
from jax.sharding import PartitionSpec as P

NORM_EPS = 1e-6
WHITEN_EPS = 1e-8
DISCOUNT = 1.0
GAE_LAMBDA = 0.995
MESH = pl.DeviceIdType.MESH

ROWS, PIECE, CP, DP = 16, 32, 4, 2
SEQ = PIECE * CP
TOK = ROWS * PIECE
HALF = TOK // 2
SEND_CHUNKS = 4
FC = 256
SLOTS = 8
VARIANTS = (192, 224, 256, 288, 320, 384, 448, 512)


def iota(shape, dim):
    return lax.broadcasted_iota(jnp.int32, shape, dim)


def everyone(dp, cp):
    for step in range(1, DP * CP):
        yield lax.rem(dp + step // CP, DP), lax.rem(cp + step % CP, CP)


def token_row(placed):
    spread = (lax.rem(iota((SEQ, TOK), 0), PIECE) == lax.rem(iota((SEQ, TOK), 1), PIECE)).astype(jnp.bfloat16)
    by_row = jnp.dot(placed.astype(jnp.bfloat16), spread, preferred_element_type=jnp.float32)
    own = iota((ROWS, TOK), 0) == iota((ROWS, TOK), 1) // PIECE
    return jnp.sum(jnp.where(own, by_row, 0.0), axis=0, keepdims=True)


def token_rank(row):
    upper = (iota((TOK, TOK), 0) <= iota((TOK, TOK), 1)).astype(jnp.bfloat16)
    upto = jnp.dot(jnp.broadcast_to(row, (8, TOK)).astype(jnp.bfloat16), upper, preferred_element_type=jnp.float32)[:1]
    return jnp.where(row > 0.0, upto - 1.0, -1.0)


def gather_kernel(x_hbm, mask_hbm, rew_hbm, xs_ref, tid_ref, cnt_ref, gm_ref,
                  x_v, mask_v, rew_v, sendbuf, recvbuf, pack, packs, place, in_sem, pk_send, pk_recv, x_send, x_recv):
    dp, cp = lax.axis_index('dp'), lax.axis_index('cp')
    mate = cp + 1 - 2 * lax.rem(cp, 2)
    loads = [pltpu.make_async_copy(src, dst, in_sem.at[k])
             for k, (src, dst) in enumerate(((mask_hbm, mask_v), (rew_hbm, rew_v), (x_hbm, x_v)))]
    for load in loads:
        load.start()
    barrier = pltpu.get_barrier_semaphore()
    for to in everyone(dp, cp):
        pl.semaphore_signal(barrier, inc=1, device_id=to, device_id_type=MESH)

    loads[0].wait()
    loads[1].wait()
    mask_f = mask_v[...].astype(jnp.float32)
    for half, block in enumerate((mask_f, jnp.where(mask_f > 0.0, rew_v[...], 0.0))):
        place[half] = jnp.zeros((ROWS, SEQ), jnp.float32)
        place[half, :, :PIECE] = block
        base = place[half]
        moved = base
        for piece in range(1, CP):
            moved = jnp.where(cp == piece, pltpu.roll(base, piece * PIECE, 1), moved)
        pack[half] = moved
    row = token_row(pack[0])
    rank = token_rank(row)
    pl.semaphore_wait(barrier, DP * CP - 1)

    me = dp * CP + cp
    shares = []
    for k, to in enumerate(everyone(dp, cp)):
        share = pltpu.make_async_remote_copy(
            src_ref=pack, dst_ref=packs.at[k], send_sem=pk_send.at[k], recv_sem=pk_recv.at[k],
            device_id=to, device_id_type=MESH)
        share.start()
        shares.append(share)

    loads[2].wait()
    send_rank = (2 * iota((HALF, TOK), 0) + 1).astype(jnp.float32)
    pick = (rank == send_rank).astype(jnp.bfloat16)
    width = x_v.shape[1] // SEND_CHUNKS
    moves = []
    for j in range(SEND_CHUNKS):
        cols = slice(j * width, (j + 1) * width)
        sendbuf[j] = jnp.dot(pick, x_v[:, cols], preferred_element_type=jnp.float32)
        move = pltpu.make_async_remote_copy(
            src_ref=sendbuf.at[j], dst_ref=recvbuf.at[j], send_sem=x_send.at[j], recv_sem=x_recv.at[j],
            device_id=(dp, mate), device_id_type=MESH)
        move.start()
        moves.append(move)

    for share in shares:
        share.wait_recv()
    placed = [[pack[half] for half in range(2)]] + [[packs[k, half] for half in range(2)] for k in range(DP * CP - 1)]
    same = [sum(placed[k][half] for k in range(CP)) for half in range(2)]
    other = [sum(placed[k][half] for k in range(CP, 2 * CP)) for half in range(2)]
    for half in range(2):
        gm_ref[half, :ROWS, :] = same[half]
        gm_ref[half, ROWS:, :] = other[half]
    lane = iota((ROWS, SEQ), 1)
    mate_row = token_row(jnp.where(lane // PIECE == mate, same[0], 0.0))
    mate_rank = token_rank(mate_row)
    got = jnp.floor(jnp.sum(mate_row, axis=1, keepdims=True) * 0.5)
    keep = jnp.floor((jnp.sum(row, axis=1, keepdims=True) + 1.0) * 0.5)
    cnt_ref[...] = jnp.broadcast_to(got + keep, (8, 128))

    slot = iota((TOK, TOK), 0).astype(jnp.float32)
    own = rank == 2.0 * (slot - got)
    own = jnp.logical_and(own, slot >= got)
    tok = iota((1, TOK), 1)
    code = ((tok // PIECE) * SEQ + lax.rem(tok, PIECE)).astype(jnp.float32)
    own_code = code + (cp * PIECE).astype(jnp.float32)
    mate_code = code + (mate * PIECE).astype(jnp.float32)
    theirs = mate_rank == send_rank
    tid = jnp.sum(jnp.where(own, own_code, 0.0), axis=1, keepdims=True)
    tid_ref[...] = tid.astype(jnp.int32)
    tid_ref[:HALF, :] = (tid[:HALF] + jnp.sum(jnp.where(theirs, mate_code, 0.0), axis=1, keepdims=True)).astype(jnp.int32)
    own_pick = own.astype(jnp.bfloat16)
    came = iota((HALF, width), 0).astype(jnp.float32) < got
    for j in range(SEND_CHUNKS):
        cols = slice(j * width, (j + 1) * width)
        xs_ref[:, cols] = jnp.dot(own_pick, x_v[:, cols], preferred_element_type=jnp.float32).astype(jnp.bfloat16)
    for j in range(SEND_CHUNKS):
        cols = slice(j * width, (j + 1) * width)
        moves[j].wait_recv()
        xs_ref[:HALF, cols] = jnp.where(came, recvbuf[j], xs_ref[:HALF, cols].astype(jnp.float32)).astype(jnp.bfloat16)
    for share in shares:
        share.wait_send()
    for move in moves:
        move.wait_send()


def mlp_kernel(cnt_ref, xs_ref, tid_ref, gain_hbm, final_hbm, wv_hbm, bv_ref, wg_hbm, wu_hbm, wd_hbm, out_ref,
               gain_ref, final_ref, wv_ref, wg_buf, wu_buf, wd_buf, xn, acc, inner, col, vec_sem, sems):
    model = xs_ref.shape[1]
    chunks = wd_hbm.shape[0] // FC

    def copies(i, which=(0, 1, 2)):
        slot = lax.rem(i, SLOTS)
        at = pl.ds(pl.multiple_of(i * FC, FC), FC)
        make = (lambda: pltpu.make_async_copy(wg_hbm.at[:, at], wg_buf.at[slot], sems.at[0, slot]),
                lambda: pltpu.make_async_copy(wu_hbm.at[:, at], wu_buf.at[slot], sems.at[1, slot]),
                lambda: pltpu.make_async_copy(wd_hbm.at[at, :], wd_buf.at[slot], sems.at[2, slot]))
        return [make[w]() for w in which]

    def wait(i):
        for copy in copies(i):
            copy.wait()

    def refill(i):
        @pl.when(i + SLOTS < chunks)
        def _():
            for copy in copies(i + SLOTS):
                copy.start()

    vecs = [pltpu.make_async_copy(src, dst, vec_sem.at[k]) for k, (src, dst) in
            enumerate(((gain_hbm, gain_ref), (final_hbm, final_ref), (wv_hbm, wv_ref)))]
    for vec in vecs:
        vec.start()
    for i in range(SLOTS):
        for copy in copies(jnp.int32(i)):
            copy.start()
    count = jnp.max(cnt_ref[...]).astype(jnp.int32)

    blocks = (count + 31) // 32
    for vec in vecs:
        vec.wait()

    def norm(b, _):
        rows = pl.ds(pl.multiple_of(b * 32, 32), 32)
        x = xs_ref[rows, :].astype(jnp.float32)
        scale = lax.rsqrt(jnp.mean(x * x, axis=-1, keepdims=True) + NORM_EPS)
        xn[rows, :] = (x * scale * gain_ref[...]).astype(jnp.bfloat16)
        return 0

    lax.fori_loop(0, blocks, norm, 0)

    def run(size):
        def inside(i, where):
            slot = lax.rem(i, SLOTS)
            gate = jnp.dot(xn[:size, :], wg_buf[slot], preferred_element_type=jnp.float32)
            up = jnp.dot(xn[:size, :], wu_buf[slot], preferred_element_type=jnp.float32)
            inner[:size, where * FC:(where + 1) * FC] = (jax.nn.silu(gate) * up).astype(jnp.bfloat16)

        def down(i, where):
            return jnp.dot(inner[:size, where * FC:(where + 1) * FC], wd_buf[lax.rem(i, SLOTS)],
                           preferred_element_type=jnp.float32)

        wait(jnp.int32(0))
        inside(jnp.int32(0), 0)
        acc[:size, :] = down(jnp.int32(0), 0)

        def body(j, _):
            first, second = 2 * j + 1, 2 * j + 2
            wait(first)
            wait(second)
            refill(first - 1)
            @pl.when(j > 0)
            def _():
                refill(first - 2)
            inside(first, 0)
            inside(second, 1)
            acc[:size, :] += down(first, 0) + down(second, 1)
            return 0

        lax.fori_loop(0, (chunks - 1) // 2, body, 0)

    for k, size in enumerate(VARIANTS):
        above = VARIANTS[k - 1] if k else -1
        @pl.when(jnp.logical_and(count > above, count <= size))
        def _():
            run(size)

    col[...] = jnp.zeros_like(col)
    head_vec = final_ref[...] * wv_ref[...]

    def head(b, _):
        rows = pl.ds(pl.multiple_of(b * 32, 32), 32)
        h = xs_ref[rows, :].astype(jnp.float32) + acc[rows, :]
        scale = lax.rsqrt(jnp.mean(h * h, axis=-1, keepdims=True) + NORM_EPS)
        val = jnp.sum(h * head_vec, axis=-1, keepdims=True) * scale + bv_ref[0]
        val = jnp.where(iota((32, 1), 0) + b * 32 < count, val, 0.0)
        col[rows, :] = jnp.broadcast_to(val, (32, SEQ))
        return 0

    lax.fori_loop(0, blocks, head, 0)
    at_row = (tid_ref[...] // SEQ == iota((TOK, ROWS), 1)).astype(jnp.float32)
    at_lane = jnp.where(lax.rem(tid_ref[...], SEQ) == iota((TOK, SEQ), 1), col[...], 0.0)
    out_ref[...] = lax.dot_general(at_row, at_lane, (((0,), (0,)), ((), ())), precision=lax.Precision.HIGHEST,
                                   preferred_element_type=jnp.float32)


def share_kernel(vals_ref, all_ref, came, send, recv):
    dp, cp = lax.axis_index('dp'), lax.axis_index('cp')
    barrier = pltpu.get_barrier_semaphore()
    for to in everyone(dp, cp):
        pl.semaphore_signal(barrier, inc=1, device_id=to, device_id_type=MESH)
    pl.semaphore_wait(barrier, DP * CP - 1)
    shares = []
    for k, to in enumerate(everyone(dp, cp)):
        share = pltpu.make_async_remote_copy(
            src_ref=vals_ref, dst_ref=came.at[k], send_sem=send.at[k], recv_sem=recv.at[k],
            device_id=to, device_id_type=MESH)
        share.start()
        shares.append(share)
    for share in shares:
        share.wait_recv()
    all_ref[:ROWS, :] = vals_ref[...] + came[0] + came[1] + came[2]
    all_ref[ROWS:, :] = came[3] + came[4] + came[5] + came[6]
    for share in shares:
        share.wait_send()


def gae_kernel(vals_ref, gm_ref, v_ref, ret_ref, white_ref):
    cp = lax.axis_index('cp')
    values = vals_ref[...]
    mask, rew = gm_ref[0], gm_ref[1]
    lane = iota((2 * ROWS, SEQ), 1)

    def ahead(z, step):
        return jnp.where(lane < SEQ - step, pltpu.roll(z, SEQ - step, 1), 0.0)

    adv = rew + DISCOUNT * ahead(values, 1) - values
    step = 1
    while step < SEQ:
        adv = adv + math.pow(DISCOUNT * GAE_LAMBDA, step) * ahead(adv, step)
        step *= 2

    def total(z):
        return jnp.sum(jnp.sum(z, axis=0, keepdims=True), axis=1, keepdims=True)

    count = total(mask)
    mean = total(mask * adv) / count
    var = total(mask * adv * adv) / count - mean * mean
    white = mask * (adv - mean) * lax.rsqrt(var + WHITEN_EPS)
    for out, z in ((v_ref, values), (ret_ref, mask * (adv + values)), (white_ref, white)):
        mine = z[:ROWS]
        moved = mine
        for piece in range(1, CP):
            moved = jnp.where(cp == piece, pltpu.roll(mine, SEQ - piece * PIECE, 1), moved)
        out[...] = moved[:, :PIECE]


def vmem():
    return pl.BlockSpec(memory_space=pltpu.VMEM)


def smem():
    return pl.BlockSpec(memory_space=pltpu.SMEM)


def hbm():
    return pl.BlockSpec(memory_space=pl.ANY)


def solution(mesh):
    def local_step(x_blk, norm_gain, w_gate, w_up, w_down, final_gain, w_value, b_value, rew_blk, mask_blk):
        rows, piece, model = x_blk.shape
        f32, bf16 = jnp.float32, jnp.bfloat16
        x = x_blk.reshape(TOK, model)
        width = model // SEND_CHUNKS
        xs, tid, cnt, gm = pl.pallas_call(
            gather_kernel,
            name='gather_tokens',
            out_shape=(jax.ShapeDtypeStruct((TOK, model), bf16), jax.ShapeDtypeStruct((TOK, 1), jnp.int32),
                       jax.ShapeDtypeStruct((8, 128), f32), jax.ShapeDtypeStruct((2, DP * ROWS, SEQ), f32)),
            in_specs=[hbm(), hbm(), hbm()],
            out_specs=(vmem(),) * 4,
            scratch_shapes=[
                pltpu.VMEM((TOK, model), bf16),
                pltpu.VMEM((rows, piece), jnp.int32), pltpu.VMEM((rows, piece), f32),
                pltpu.VMEM((SEND_CHUNKS, HALF, width), f32), pltpu.VMEM((SEND_CHUNKS, HALF, width), f32),
                pltpu.VMEM((2, ROWS, SEQ), f32), pltpu.VMEM((DP * CP - 1, 2, ROWS, SEQ), f32),
                pltpu.VMEM((2, ROWS, SEQ), f32),
                pltpu.SemaphoreType.DMA((3,)),
                pltpu.SemaphoreType.DMA((DP * CP - 1,)), pltpu.SemaphoreType.DMA((DP * CP - 1,)),
                pltpu.SemaphoreType.DMA((SEND_CHUNKS,)), pltpu.SemaphoreType.DMA((SEND_CHUNKS,)),
            ],
            compiler_params=pltpu.CompilerParams(collective_id=0, has_side_effects=True, vmem_limit_bytes=40 << 20),
        )(*(pltpu.with_memory_space_constraint(z, pltpu.HBM) for z in (x, mask_blk, rew_blk)))
        vals = pl.pallas_call(
            mlp_kernel,
            name='active_mlp',
            out_shape=jax.ShapeDtypeStruct((ROWS, SEQ), f32),
            in_specs=[vmem(), vmem(), vmem(), hbm(), hbm(), hbm(), smem(), hbm(), hbm(), hbm()],
            out_specs=vmem(),
            scratch_shapes=[
                pltpu.VMEM((1, model), f32), pltpu.VMEM((1, model), f32), pltpu.VMEM((1, model), f32),
                pltpu.VMEM((SLOTS, model, FC), bf16), pltpu.VMEM((SLOTS, model, FC), bf16),
                pltpu.VMEM((SLOTS, FC, model), bf16),
                pltpu.VMEM((TOK, model), bf16), pltpu.VMEM((TOK, model), f32), pltpu.VMEM((TOK, 2 * FC), bf16),
                pltpu.VMEM((TOK, SEQ), f32),
                pltpu.SemaphoreType.DMA((3,)), pltpu.SemaphoreType.DMA((3, SLOTS)),
            ],
            compiler_params=pltpu.CompilerParams(vmem_limit_bytes=44 << 20),
        )(cnt, xs, tid, *(pltpu.with_memory_space_constraint(z.reshape(1, model), pltpu.HBM)
                          for z in (norm_gain, final_gain, w_value)), b_value.reshape(1),
          w_gate, w_up, w_down)
        both = pl.pallas_call(
            share_kernel,
            name='share_values',
            out_shape=jax.ShapeDtypeStruct((DP * ROWS, SEQ), f32),
            in_specs=[vmem()],
            out_specs=vmem(),
            scratch_shapes=[
                pltpu.VMEM((DP * CP - 1, ROWS, SEQ), f32),
                pltpu.SemaphoreType.DMA((DP * CP - 1,)), pltpu.SemaphoreType.DMA((DP * CP - 1,)),
            ],
            compiler_params=pltpu.CompilerParams(collective_id=1, has_side_effects=True, vmem_limit_bytes=4 << 20),
        )(vals)
        block = jax.ShapeDtypeStruct((rows, piece), f32)
        return pl.pallas_call(
            gae_kernel,
            name='gae',
            out_shape=(block, block, block),
            in_specs=[vmem(), vmem()],
            out_specs=(vmem(),) * 3,
            compiler_params=pltpu.CompilerParams(vmem_limit_bytes=4 << 20),
        )(both, gm)

    tok_spec = P('dp', 'cp')
    in_specs = (P('dp', 'cp', None), P(None), P(None, None), P(None, None), P(None, None), P(None), P(None), P(),
                tok_spec, tok_spec)
    return jax.shard_map(local_step, mesh=mesh, in_specs=in_specs, out_specs=(tok_spec,) * 3, check_vma=False)
```

```python
import functools
import math

import jax
import jax.numpy as jnp
from jax import lax
from jax.experimental import pallas as pl
from jax.experimental.pallas import tpu as pltpu
from jax.sharding import PartitionSpec as P

NORM_EPS = 1e-6
WHITEN_EPS = 1e-8
DISCOUNT = 1.0
GAE_LAMBDA = 0.995
MESH = pl.DeviceIdType.MESH

ROWS, PIECE, CP, DP = 16, 32, 4, 2
SEQ = PIECE * CP
TOK = ROWS * PIECE
HALF = TOK // 2
SEND_CHUNKS = 4
FC = 256
SLOTS = 9
EARLY = 6
VARIANTS = (192, 224, 256, 288, 320, 384, 448, 512)


def iota(shape, dim):
    return lax.broadcasted_iota(jnp.int32, shape, dim)


def everyone(dp, cp):
    for step in range(1, DP * CP):
        yield lax.rem(dp + step // CP, DP), lax.rem(cp + step % CP, CP)


def token_row(placed):
    spread = (lax.rem(iota((SEQ, TOK), 0), PIECE) == lax.rem(iota((SEQ, TOK), 1), PIECE)).astype(jnp.bfloat16)
    by_row = jnp.dot(placed.astype(jnp.bfloat16), spread, preferred_element_type=jnp.float32)
    own = iota((ROWS, TOK), 0) == iota((ROWS, TOK), 1) // PIECE
    return jnp.sum(jnp.where(own, by_row, 0.0), axis=0, keepdims=True)


def token_rank(row):
    upper = (iota((TOK, TOK), 0) <= iota((TOK, TOK), 1)).astype(jnp.bfloat16)
    upto = jnp.dot(jnp.broadcast_to(row, (8, TOK)).astype(jnp.bfloat16), upper, preferred_element_type=jnp.float32)[:1]
    return jnp.where(row > 0.0, upto - 1.0, -1.0)


def weight_copies(i, hbm_refs, slots, sems, which=(0, 1, 2)):
    slot = lax.rem(i, SLOTS)
    at = pl.ds(pl.multiple_of(i * FC, FC), FC)
    return [pltpu.make_async_copy(hbm_refs[w].at[at, :] if w == 2 else hbm_refs[w].at[:, at], slots[w].at[slot],
                                  sems.at[w, slot]) for w in which]


def gather_kernel(x_hbm, mask_hbm, rew_hbm, wg_hbm, wu_hbm, wd_hbm,
                  xs_ref, tid_ref, cnt_ref, gm_ref, wg_buf, wu_buf, wd_buf,
                  x_v, mask_v, rew_v, sendbuf, recvbuf, pack, packs, place, w_sems, in_sem, pk_send, pk_recv, x_send, x_recv):
    dp, cp = lax.axis_index('dp'), lax.axis_index('cp')
    mate = cp + 1 - 2 * lax.rem(cp, 2)
    loads = [pltpu.make_async_copy(src, dst, in_sem.at[k])
             for k, (src, dst) in enumerate(((mask_hbm, mask_v), (rew_hbm, rew_v), (x_hbm, x_v)))]
    for load in loads:
        load.start()
    early = [copy for i in range(EARLY) for copy in
             weight_copies(i, (wg_hbm, wu_hbm, wd_hbm), (wg_buf, wu_buf, wd_buf), w_sems)]
    for copy in early:
        copy.start()
    barrier = pltpu.get_barrier_semaphore()
    for to in everyone(dp, cp):
        pl.semaphore_signal(barrier, inc=1, device_id=to, device_id_type=MESH)

    loads[0].wait()
    loads[1].wait()
    mask_f = mask_v[...].astype(jnp.float32)
    for half, block in enumerate((mask_f, jnp.where(mask_f > 0.0, rew_v[...], 0.0))):
        place[half] = jnp.zeros((ROWS, SEQ), jnp.float32)
        place[half, :, :PIECE] = block
        base = place[half]
        moved = base
        for piece in range(1, CP):
            moved = jnp.where(cp == piece, pltpu.roll(base, piece * PIECE, 1), moved)
        pack[half] = moved
    row = token_row(pack[0])
    rank = token_rank(row)
    pl.semaphore_wait(barrier, DP * CP - 1)

    me = dp * CP + cp
    shares = []
    for k, to in enumerate(everyone(dp, cp)):
        share = pltpu.make_async_remote_copy(
            src_ref=pack, dst_ref=packs.at[k], send_sem=pk_send.at[k], recv_sem=pk_recv.at[k],
            device_id=to, device_id_type=MESH)
        share.start()
        shares.append(share)

    loads[2].wait()
    send_rank = (2 * iota((HALF, TOK), 0) + 1).astype(jnp.float32)
    pick = (rank == send_rank).astype(jnp.bfloat16)
    width = x_v.shape[1] // SEND_CHUNKS
    moves = []
    for j in range(SEND_CHUNKS):
        cols = slice(j * width, (j + 1) * width)
        sendbuf[j] = jnp.dot(pick, x_v[:, cols], preferred_element_type=jnp.float32)
        move = pltpu.make_async_remote_copy(
            src_ref=sendbuf.at[j], dst_ref=recvbuf.at[j], send_sem=x_send.at[j], recv_sem=x_recv.at[j],
            device_id=(dp, mate), device_id_type=MESH)
        move.start()
        moves.append(move)

    for share in shares:
        share.wait_recv()
    placed = [[pack[half] for half in range(2)]] + [[packs[k, half] for half in range(2)] for k in range(DP * CP - 1)]
    same = [sum(placed[k][half] for k in range(CP)) for half in range(2)]
    other = [sum(placed[k][half] for k in range(CP, 2 * CP)) for half in range(2)]
    for half in range(2):
        gm_ref[half, :ROWS, :] = same[half]
        gm_ref[half, ROWS:, :] = other[half]
    lane = iota((ROWS, SEQ), 1)
    mate_row = token_row(jnp.where(lane // PIECE == mate, same[0], 0.0))
    mate_rank = token_rank(mate_row)
    got = jnp.floor(jnp.sum(mate_row, axis=1, keepdims=True) * 0.5)
    keep = jnp.floor((jnp.sum(row, axis=1, keepdims=True) + 1.0) * 0.5)
    cnt_ref[...] = jnp.broadcast_to(got + keep, (8, 128))

    slot = iota((TOK, TOK), 0).astype(jnp.float32)
    own = rank == 2.0 * (slot - got)
    own = jnp.logical_and(own, slot >= got)
    tok = iota((1, TOK), 1)
    code = ((tok // PIECE) * SEQ + lax.rem(tok, PIECE)).astype(jnp.float32)
    own_code = code + (cp * PIECE).astype(jnp.float32)
    mate_code = code + (mate * PIECE).astype(jnp.float32)
    theirs = mate_rank == send_rank
    tid = jnp.sum(jnp.where(own, own_code, 0.0), axis=1, keepdims=True)
    tid_ref[...] = tid.astype(jnp.int32)
    tid_ref[:HALF, :] = (tid[:HALF] + jnp.sum(jnp.where(theirs, mate_code, 0.0), axis=1, keepdims=True)).astype(jnp.int32)
    own_pick = own.astype(jnp.bfloat16)
    came = iota((HALF, width), 0).astype(jnp.float32) < got
    for j in range(SEND_CHUNKS):
        cols = slice(j * width, (j + 1) * width)
        xs_ref[:, cols] = jnp.dot(own_pick, x_v[:, cols], preferred_element_type=jnp.float32).astype(jnp.bfloat16)
    for j in range(SEND_CHUNKS):
        cols = slice(j * width, (j + 1) * width)
        moves[j].wait_recv()
        xs_ref[:HALF, cols] = jnp.where(came, recvbuf[j], xs_ref[:HALF, cols].astype(jnp.float32)).astype(jnp.bfloat16)
    for share in shares:
        share.wait_send()
    for move in moves:
        move.wait_send()
    for copy in early:
        copy.wait()


def mlp_kernel(cnt_ref, xs_ref, tid_ref, gain_hbm, final_hbm, wv_hbm, bv_ref, wg_hbm, wu_hbm, wd_hbm,
               wg_in, wu_in, wd_in, out_ref, wg_buf, wu_buf, wd_buf,
               gain_ref, final_ref, wv_ref, xn, acc, inner, col, vec_sem, sems):
    chunks = wd_hbm.shape[0] // FC

    def copies(i):
        return weight_copies(i, (wg_hbm, wu_hbm, wd_hbm), (wg_buf, wu_buf, wd_buf), sems)

    def wait(i):
        @pl.when(i >= EARLY)
        def _():
            for copy in copies(i):
                copy.wait()

    def refill(i):
        @pl.when(i + SLOTS < chunks)
        def _():
            for copy in copies(i + SLOTS):
                copy.start()

    vecs = [pltpu.make_async_copy(src, dst, vec_sem.at[k]) for k, (src, dst) in
            enumerate(((gain_hbm, gain_ref), (final_hbm, final_ref), (wv_hbm, wv_ref)))]
    for vec in vecs:
        vec.start()
    for i in range(EARLY, SLOTS):
        for copy in copies(i):
            copy.start()
    count = jnp.max(cnt_ref[...]).astype(jnp.int32)

    blocks = (count + 31) // 32
    for vec in vecs:
        vec.wait()

    def norm(b, _):
        rows = pl.ds(pl.multiple_of(b * 32, 32), 32)
        x = xs_ref[rows, :].astype(jnp.float32)
        scale = lax.rsqrt(jnp.mean(x * x, axis=-1, keepdims=True) + NORM_EPS)
        xn[rows, :] = (x * scale * gain_ref[...]).astype(jnp.bfloat16)
        return 0

    lax.fori_loop(0, blocks, norm, 0)

    model = xs_ref.shape[1]
    quarters = [slice(q * model // 4, (q + 1) * model // 4) for q in range(4)]

    def run(size):
        def inside(i, where):
            slot = lax.rem(i, SLOTS)
            gate = jnp.dot(xn[:size, :], wg_buf[slot], preferred_element_type=jnp.float32)
            up = jnp.dot(xn[:size, :], wu_buf[slot], preferred_element_type=jnp.float32)
            inner[:size, where * FC:(where + 1) * FC] = (jax.nn.silu(gate) * up).astype(jnp.bfloat16)

        def down(i, where, cols):
            return jnp.dot(inner[:size, where * FC:(where + 1) * FC], wd_buf[lax.rem(i, SLOTS), :, cols],
                           preferred_element_type=jnp.float32)

        inside(0, 0)
        for cols in quarters:
            acc[:size, cols] = down(0, 0, cols)

        def body(j, _):
            first, second = 2 * j + 1, 2 * j + 2
            wait(first)
            wait(second)
            refill(first - 1)
            @pl.when(j > 0)
            def _():
                refill(first - 2)
            inside(first, 0)
            inside(second, 1)
            for cols in quarters:
                acc[:size, cols] += down(first, 0, cols) + down(second, 1, cols)
            return 0

        lax.fori_loop(0, (chunks - 1) // 2, body, 0)

    for k, size in enumerate(VARIANTS):
        above = VARIANTS[k - 1] if k else -1
        @pl.when(jnp.logical_and(count > above, count <= size))
        def _():
            run(size)

    col[...] = jnp.zeros_like(col)
    head_vec = final_ref[...] * wv_ref[...]

    def head(b, _):
        rows = pl.ds(pl.multiple_of(b * 32, 32), 32)
        h = xs_ref[rows, :].astype(jnp.float32) + acc[rows, :]
        scale = lax.rsqrt(jnp.mean(h * h, axis=-1, keepdims=True) + NORM_EPS)
        val = jnp.sum(h * head_vec, axis=-1, keepdims=True) * scale + bv_ref[0]
        val = jnp.where(iota((32, 1), 0) + b * 32 < count, val, 0.0)
        col[rows, :] = jnp.broadcast_to(val, (32, SEQ))
        return 0

    lax.fori_loop(0, blocks, head, 0)
    at_row = (tid_ref[...] // SEQ == iota((TOK, ROWS), 1)).astype(jnp.float32)
    at_lane = jnp.where(lax.rem(tid_ref[...], SEQ) == iota((TOK, SEQ), 1), col[...], 0.0)
    out_ref[...] = lax.dot_general(at_row, at_lane, (((0,), (0,)), ((), ())), precision=lax.Precision.HIGHEST,
                                   preferred_element_type=jnp.float32)


def share_kernel(vals_ref, all_ref, came, send, recv):
    dp, cp = lax.axis_index('dp'), lax.axis_index('cp')
    barrier = pltpu.get_barrier_semaphore()
    for to in everyone(dp, cp):
        pl.semaphore_signal(barrier, inc=1, device_id=to, device_id_type=MESH)
    pl.semaphore_wait(barrier, DP * CP - 1)
    shares = []
    for k, to in enumerate(everyone(dp, cp)):
        share = pltpu.make_async_remote_copy(
            src_ref=vals_ref, dst_ref=came.at[k], send_sem=send.at[k], recv_sem=recv.at[k],
            device_id=to, device_id_type=MESH)
        share.start()
        shares.append(share)
    for share in shares:
        share.wait_recv()
    all_ref[:ROWS, :] = vals_ref[...] + came[0] + came[1] + came[2]
    all_ref[ROWS:, :] = came[3] + came[4] + came[5] + came[6]
    for share in shares:
        share.wait_send()


def gae_kernel(vals_ref, gm_ref, v_ref, ret_ref, white_ref):
    cp = lax.axis_index('cp')
    values = vals_ref[...]
    mask, rew = gm_ref[0], gm_ref[1]
    lane = iota((2 * ROWS, SEQ), 1)

    def ahead(z, step):
        return jnp.where(lane < SEQ - step, pltpu.roll(z, SEQ - step, 1), 0.0)

    adv = rew + DISCOUNT * ahead(values, 1) - values
    step = 1
    while step < SEQ:
        adv = adv + math.pow(DISCOUNT * GAE_LAMBDA, step) * ahead(adv, step)
        step *= 2

    def total(z):
        return jnp.sum(jnp.sum(z, axis=0, keepdims=True), axis=1, keepdims=True)

    count = total(mask)
    mean = total(mask * adv) / count
    var = total(mask * adv * adv) / count - mean * mean
    white = mask * (adv - mean) * lax.rsqrt(var + WHITEN_EPS)
    for out, z in ((v_ref, values), (ret_ref, mask * (adv + values)), (white_ref, white)):
        mine = z[:ROWS]
        moved = mine
        for piece in range(1, CP):
            moved = jnp.where(cp == piece, pltpu.roll(mine, SEQ - piece * PIECE, 1), moved)
        out[...] = moved[:, :PIECE]


def vmem():
    return pl.BlockSpec(memory_space=pltpu.VMEM)


def smem():
    return pl.BlockSpec(memory_space=pltpu.SMEM)


def hbm():
    return pl.BlockSpec(memory_space=pl.ANY)


def solution(mesh):
    def local_step(x_blk, norm_gain, w_gate, w_up, w_down, final_gain, w_value, b_value, rew_blk, mask_blk):
        rows, piece, model = x_blk.shape
        f32, bf16 = jnp.float32, jnp.bfloat16
        x = x_blk.reshape(TOK, model)
        width = model // SEND_CHUNKS
        slot_shapes = tuple(jax.ShapeDtypeStruct((SLOTS,) + z, bf16) for z in ((model, FC), (model, FC), (FC, model)))
        xs, tid, cnt, gm, *slots = pl.pallas_call(
            gather_kernel,
            name='gather_tokens',
            out_shape=(jax.ShapeDtypeStruct((TOK, model), bf16), jax.ShapeDtypeStruct((TOK, 1), jnp.int32),
                       jax.ShapeDtypeStruct((8, 128), f32), jax.ShapeDtypeStruct((2, DP * ROWS, SEQ), f32)) + slot_shapes,
            in_specs=[hbm()] * 6,
            out_specs=(vmem(),) * 7,
            scratch_shapes=[
                pltpu.VMEM((TOK, model), bf16),
                pltpu.VMEM((rows, piece), jnp.int32), pltpu.VMEM((rows, piece), f32),
                pltpu.VMEM((SEND_CHUNKS, HALF, width), f32), pltpu.VMEM((SEND_CHUNKS, HALF, width), f32),
                pltpu.VMEM((2, ROWS, SEQ), f32), pltpu.VMEM((DP * CP - 1, 2, ROWS, SEQ), f32),
                pltpu.VMEM((2, ROWS, SEQ), f32),
                pltpu.SemaphoreType.DMA((3, SLOTS)), pltpu.SemaphoreType.DMA((3,)),
                pltpu.SemaphoreType.DMA((DP * CP - 1,)), pltpu.SemaphoreType.DMA((DP * CP - 1,)),
                pltpu.SemaphoreType.DMA((SEND_CHUNKS,)), pltpu.SemaphoreType.DMA((SEND_CHUNKS,)),
            ],
            compiler_params=pltpu.CompilerParams(collective_id=0, has_side_effects=True, vmem_limit_bytes=16 << 20),
        )(*(pltpu.with_memory_space_constraint(z, pltpu.HBM) for z in (x, mask_blk, rew_blk, w_gate, w_up, w_down)))
        vals, *_ = pl.pallas_call(
            mlp_kernel,
            name='active_mlp',
            out_shape=(jax.ShapeDtypeStruct((ROWS, SEQ), f32),) + slot_shapes,
            in_specs=[vmem()] * 3 + [hbm()] * 3 + [smem()] + [hbm()] * 3 + [vmem()] * 3,
            out_specs=(vmem(),) * 4,
            input_output_aliases={10: 1, 11: 2, 12: 3},
            scratch_shapes=[
                pltpu.VMEM((1, model), f32), pltpu.VMEM((1, model), f32), pltpu.VMEM((1, model), f32),
                pltpu.VMEM((TOK, model), bf16), pltpu.VMEM((TOK, model), f32), pltpu.VMEM((TOK, 2 * FC), bf16),
                pltpu.VMEM((TOK, SEQ), f32),
                pltpu.SemaphoreType.DMA((3,)), pltpu.SemaphoreType.DMA((3, SLOTS)),
            ],
            compiler_params=pltpu.CompilerParams(vmem_limit_bytes=18 << 20),
        )(cnt, xs, tid, *(pltpu.with_memory_space_constraint(z.reshape(1, model), pltpu.HBM)
                          for z in (norm_gain, final_gain, w_value)), b_value.reshape(1),
          *(pltpu.with_memory_space_constraint(z, pltpu.HBM) for z in (w_gate, w_up, w_down)), *slots)
        both = pl.pallas_call(
            share_kernel,
            name='share_values',
            out_shape=jax.ShapeDtypeStruct((DP * ROWS, SEQ), f32),
            in_specs=[vmem()],
            out_specs=vmem(),
            scratch_shapes=[
                pltpu.VMEM((DP * CP - 1, ROWS, SEQ), f32),
                pltpu.SemaphoreType.DMA((DP * CP - 1,)), pltpu.SemaphoreType.DMA((DP * CP - 1,)),
            ],
            compiler_params=pltpu.CompilerParams(collective_id=1, has_side_effects=True, vmem_limit_bytes=4 << 20),
        )(vals)
        block = jax.ShapeDtypeStruct((rows, piece), f32)
        return pl.pallas_call(
            gae_kernel,
            name='gae',
            out_shape=(block, block, block),
            in_specs=[vmem(), vmem()],
            out_specs=(vmem(),) * 3,
            compiler_params=pltpu.CompilerParams(vmem_limit_bytes=4 << 20),
        )(both, gm)

    tok_spec = P('dp', 'cp')
    in_specs = (P('dp', 'cp', None), P(None), P(None, None), P(None, None), P(None, None), P(None), P(None), P(),
                tok_spec, tok_spec)
    return jax.shard_map(local_step, mesh=mesh, in_specs=in_specs, out_specs=(tok_spec,) * 3, check_vma=False)
```

```python
import functools
import math

import jax
import jax.numpy as jnp
from jax import lax
from jax.experimental import pallas as pl
from jax.experimental.pallas import tpu as pltpu
from jax.sharding import PartitionSpec as P

NORM_EPS = 1e-6
WHITEN_EPS = 1e-8
DISCOUNT = 1.0
GAE_LAMBDA = 0.995
MESH = pl.DeviceIdType.MESH

ROWS, PIECE, CP, DP = 16, 32, 4, 2
SEQ = PIECE * CP
TOK = ROWS * PIECE
HALF = TOK // 2
SEND_CHUNKS = 4
FC = 256
SLOTS = 10
EARLY = 7
UNIT = 3
SIZES = tuple(range(192, 321, 16))
BLOCK = 64


def iota(shape, dim):
    return lax.broadcasted_iota(jnp.int32, shape, dim)


def everyone(dp, cp):
    for step in range(1, DP * CP):
        yield lax.rem(dp + step // CP, DP), lax.rem(cp + step % CP, CP)


def token_row(placed):
    spread = (lax.rem(iota((SEQ, TOK), 0), PIECE) == lax.rem(iota((SEQ, TOK), 1), PIECE)).astype(jnp.bfloat16)
    by_row = jnp.dot(placed.astype(jnp.bfloat16), spread, preferred_element_type=jnp.float32)
    own = iota((ROWS, TOK), 0) == iota((ROWS, TOK), 1) // PIECE
    return jnp.sum(jnp.where(own, by_row, 0.0), axis=0, keepdims=True)


def token_rank(row):
    upper = (iota((TOK, TOK), 0) <= iota((TOK, TOK), 1)).astype(jnp.bfloat16)
    upto = jnp.dot(jnp.broadcast_to(row, (8, TOK)).astype(jnp.bfloat16), upper, preferred_element_type=jnp.float32)[:1]
    return jnp.where(row > 0.0, upto - 1.0, -1.0)


def weight_copies(chunk, slot, hbm_refs, slots, sems):
    at = pl.ds(pl.multiple_of(chunk * FC, FC), FC)
    return [pltpu.make_async_copy(hbm_refs[w].at[at, :] if w == 2 else hbm_refs[w].at[:, at], slots[w].at[slot],
                                  sems.at[w, slot]) for w in range(3)]


def gather_kernel(x_hbm, mask_hbm, rew_hbm, wg_hbm, wu_hbm, wd_hbm,
                  xs_ref, code_ref, cnt_ref, gm_ref, wg_buf, wu_buf, wd_buf,
                  x_v, mask_v, rew_v, sendbuf, recvbuf, pack, packs, place, w_sems, in_sem, pk_send, pk_recv, x_send, x_recv):
    dp, cp = lax.axis_index('dp'), lax.axis_index('cp')
    mate = cp + 1 - 2 * lax.rem(cp, 2)
    loads = [pltpu.make_async_copy(src, dst, in_sem.at[k])
             for k, (src, dst) in enumerate(((mask_hbm, mask_v), (rew_hbm, rew_v), (x_hbm, x_v)))]
    for load in loads:
        load.start()
    early = [copy for i in range(EARLY) for copy in
             weight_copies(i, i, (wg_hbm, wu_hbm, wd_hbm), (wg_buf, wu_buf, wd_buf), w_sems)]
    for copy in early:
        copy.start(priority=1)
    barrier = pltpu.get_barrier_semaphore()
    for to in everyone(dp, cp):
        pl.semaphore_signal(barrier, inc=1, device_id=to, device_id_type=MESH)

    loads[0].wait()
    loads[1].wait()
    mask_f = mask_v[...].astype(jnp.float32)
    for half, block in enumerate((mask_f, jnp.where(mask_f > 0.0, rew_v[...], 0.0))):
        place[half] = jnp.zeros((ROWS, SEQ), jnp.float32)
        place[half, :, :PIECE] = block
        base = place[half]
        moved = base
        for piece in range(1, CP):
            moved = jnp.where(cp == piece, pltpu.roll(base, piece * PIECE, 1), moved)
        pack[half] = moved
    row = token_row(pack[0])
    rank = token_rank(row)
    pl.semaphore_wait(barrier, DP * CP - 1)

    me = dp * CP + cp
    shares = []
    for k, to in enumerate(everyone(dp, cp)):
        share = pltpu.make_async_remote_copy(
            src_ref=pack, dst_ref=packs.at[k], send_sem=pk_send.at[k], recv_sem=pk_recv.at[k],
            device_id=to, device_id_type=MESH)
        share.start()
        shares.append(share)

    loads[2].wait()
    send_rank = (2 * iota((HALF, TOK), 0) + 1).astype(jnp.float32)
    pick = (rank == send_rank).astype(jnp.bfloat16)
    width = x_v.shape[1] // SEND_CHUNKS
    moves = []
    for j in range(SEND_CHUNKS):
        cols = slice(j * width, (j + 1) * width)
        sendbuf[j] = jnp.dot(pick, x_v[:, cols], preferred_element_type=jnp.float32)
        move = pltpu.make_async_remote_copy(
            src_ref=sendbuf.at[j], dst_ref=recvbuf.at[j], send_sem=x_send.at[j], recv_sem=x_recv.at[j],
            device_id=(dp, mate), device_id_type=MESH)
        move.start()
        moves.append(move)

    for share in shares:
        share.wait_recv()
    placed = [[pack[half] for half in range(2)]] + [[packs[k, half] for half in range(2)] for k in range(DP * CP - 1)]
    same = [sum(placed[k][half] for k in range(CP)) for half in range(2)]
    other = [sum(placed[k][half] for k in range(CP, 2 * CP)) for half in range(2)]
    for half in range(2):
        gm_ref[half, :ROWS, :] = same[half]
        gm_ref[half, ROWS:, :] = other[half]
    lane = iota((ROWS, SEQ), 1)
    mate_row = token_row(jnp.where(lane // PIECE == mate, same[0], 0.0))
    mate_rank = token_rank(mate_row)
    got = jnp.floor(jnp.sum(mate_row, axis=1, keepdims=True) * 0.5)
    keep = jnp.floor((jnp.sum(row, axis=1, keepdims=True) + 1.0) * 0.5)
    cnt_ref[...] = jnp.broadcast_to(got + keep, (8, 128))

    slot = iota((TOK, TOK), 0).astype(jnp.float32)
    own = jnp.logical_and(rank == 2.0 * (slot - got), slot >= got).astype(jnp.bfloat16)
    theirs = (mate_rank == send_rank).astype(jnp.bfloat16)
    tok, half = iota((TOK, 2 * SEQ), 0), iota((TOK, 2 * SEQ), 1) // SEQ

    def codes(pick, piece):
        parts = jnp.where(half == 0, tok // PIECE, lax.rem(tok, PIECE) + piece * PIECE)
        parts = jnp.dot(pick, parts.astype(jnp.float32).astype(jnp.bfloat16), preferred_element_type=jnp.float32)
        return parts[:, :SEQ] * SEQ + parts[:, SEQ:]

    code = codes(own, cp)
    code_ref[...] = code
    code_ref[:HALF, :] = code[:HALF] + codes(theirs, mate)
    came = iota((HALF, width), 0).astype(jnp.float32) < got
    for j in range(SEND_CHUNKS):
        cols = slice(j * width, (j + 1) * width)
        xs_ref[:, cols] = jnp.dot(own, x_v[:, cols], preferred_element_type=jnp.float32).astype(jnp.bfloat16)
    for j in range(SEND_CHUNKS):
        cols = slice(j * width, (j + 1) * width)
        moves[j].wait_recv()
        xs_ref[:HALF, cols] = jnp.where(came, recvbuf[j], xs_ref[:HALF, cols].astype(jnp.float32)).astype(jnp.bfloat16)
    for share in shares:
        share.wait_send()
    for move in moves:
        move.wait_send()
    for copy in early:
        copy.wait()


def mlp_kernel(cnt_ref, xs_ref, code_ref, gain_hbm, final_hbm, wv_hbm, bv_ref, wg_hbm, wu_hbm, wd_hbm,
               wg_in, wu_in, wd_in, out_ref, wg_buf, wu_buf, wd_buf,
               gain_ref, final_ref, wv_ref, xn, acc, inner, col, vec_sem, sems):
    chunks = wd_hbm.shape[0] // FC
    model = xs_ref.shape[1]
    quarters = [slice(q * model // 4, (q + 1) * model // 4) for q in range(4)]

    def copies(i):
        return weight_copies(lax.rem(i, chunks), lax.rem(i, SLOTS), (wg_hbm, wu_hbm, wd_hbm), (wg_buf, wu_buf, wd_buf), sems)

    vecs = [pltpu.make_async_copy(src, dst, vec_sem.at[k]) for k, (src, dst) in
            enumerate(((gain_hbm, gain_ref), (final_hbm, final_ref), (wv_hbm, wv_ref)))]
    for vec in vecs:
        vec.start()
    for i in range(EARLY, SLOTS):
        for copy in copies(i):
            copy.start(priority=1)
    count = jnp.max(cnt_ref[...]).astype(jnp.int32)
    passes = jnp.where(count > SIZES[-1], 2, 1)
    per = jnp.where(count > SIZES[-1], (count + 63) // 64 * 32, count)
    blocks = (count + BLOCK - 1) // BLOCK

    def wait(i):
        @pl.when(i >= EARLY)
        def _():
            for copy in copies(i):
                copy.wait()

    def refill(i):
        @pl.when(i + SLOTS < passes * chunks)
        def _():
            for copy in copies(i + SLOTS):
                copy.start(priority=1)

    for vec in vecs:
        vec.wait()

    def norm(b, _):
        rows = pl.ds(pl.multiple_of(b * BLOCK, BLOCK), BLOCK)
        x = xs_ref[rows, :].astype(jnp.float32)
        scale = lax.rsqrt(jnp.mean(x * x, axis=-1, keepdims=True) + NORM_EPS)
        xn[rows, :] = (x * scale * gain_ref[...]).astype(jnp.bfloat16)
        return 0

    lax.fori_loop(0, blocks, norm, 0)

    def run(size, p):
        rows = pl.ds(pl.multiple_of(p * per, 32), size)
        begin = p * chunks

        def inside(i, where):
            slot = lax.rem(i, SLOTS)
            gate = jnp.dot(xn[rows, :], wg_buf[slot], preferred_element_type=jnp.float32)
            up = jnp.dot(xn[rows, :], wu_buf[slot], preferred_element_type=jnp.float32)
            inner[:size, where * FC:(where + 1) * FC] = (jax.nn.silu(gate) * up).astype(jnp.bfloat16)

        def down(i, where, cols):
            return jnp.dot(inner[:size, where * FC:(where + 1) * FC], wd_buf[lax.rem(i, SLOTS), :, cols],
                           preferred_element_type=jnp.float32)

        @pl.when(p > 0)
        def _():
            for k in range(UNIT):
                refill(begin - UNIT + k)
        wait(begin)
        inside(begin, 0)
        for cols in quarters:
            acc[rows, cols] = down(begin, 0, cols)

        def body(j, _):
            unit = [begin + UNIT * j + 1 + k for k in range(UNIT)]
            for i in unit:
                wait(i)
            @pl.when(j > 0)
            def _():
                for k in range(2, UNIT + 1):
                    refill(unit[0] - k)
            refill(unit[0] - 1)
            for k, i in enumerate(unit):
                inside(i, k)
            for cols in quarters:
                acc[rows, cols] += sum(down(i, k, cols) for k, i in enumerate(unit))
            return 0

        lax.fori_loop(0, (chunks - 1) // UNIT, body, 0)

    def one_pass(p, _):
        for k, size in enumerate(SIZES):
            above = SIZES[k - 1] if k else -1
            @pl.when(jnp.logical_and(per > above, per <= size))
            def _():
                run(size, p)
        return 0

    lax.fori_loop(0, passes, one_pass, 0)

    col[...] = jnp.zeros_like(col)
    head_vec = final_ref[...] * wv_ref[...]

    def head(b, _):
        rows = pl.ds(pl.multiple_of(b * BLOCK, BLOCK), BLOCK)
        h = xs_ref[rows, :].astype(jnp.float32) + acc[rows, :]
        scale = lax.rsqrt(jnp.mean(h * h, axis=-1, keepdims=True) + NORM_EPS)
        val = jnp.sum(h * head_vec, axis=-1, keepdims=True) * scale + bv_ref[0]
        val = jnp.where(iota((BLOCK, 1), 0) + b * BLOCK < count, val, 0.0)
        col[rows, :] = jnp.broadcast_to(val, (BLOCK, SEQ))
        return 0

    lax.fori_loop(0, blocks, head, 0)
    here = iota((1, SEQ), 1).astype(jnp.float32)
    for r in range(ROWS):
        mine = jnp.where(code_ref[...] == here + r * SEQ, col[...], 0.0)
        out_ref[r:r + 1, :] = jnp.sum(mine, axis=0, keepdims=True)


def share_kernel(vals_ref, all_ref, came, send, recv):
    dp, cp = lax.axis_index('dp'), lax.axis_index('cp')
    barrier = pltpu.get_barrier_semaphore()
    for to in everyone(dp, cp):
        pl.semaphore_signal(barrier, inc=1, device_id=to, device_id_type=MESH)
    pl.semaphore_wait(barrier, DP * CP - 1)
    shares = []
    for k, to in enumerate(everyone(dp, cp)):
        share = pltpu.make_async_remote_copy(
            src_ref=vals_ref, dst_ref=came.at[k], send_sem=send.at[k], recv_sem=recv.at[k],
            device_id=to, device_id_type=MESH)
        share.start()
        shares.append(share)
    for share in shares:
        share.wait_recv()
    all_ref[:ROWS, :] = vals_ref[...] + came[0] + came[1] + came[2]
    all_ref[ROWS:, :] = came[3] + came[4] + came[5] + came[6]
    for share in shares:
        share.wait_send()


def gae_kernel(vals_ref, gm_ref, v_ref, ret_ref, white_ref):
    cp = lax.axis_index('cp')
    values = vals_ref[...]
    mask, rew = gm_ref[0], gm_ref[1]
    lane = iota((2 * ROWS, SEQ), 1)

    def ahead(z, step):
        return jnp.where(lane < SEQ - step, pltpu.roll(z, SEQ - step, 1), 0.0)

    adv = rew + DISCOUNT * ahead(values, 1) - values
    step = 1
    while step < SEQ:
        adv = adv + math.pow(DISCOUNT * GAE_LAMBDA, step) * ahead(adv, step)
        step *= 2

    def total(z):
        return jnp.sum(jnp.sum(z, axis=0, keepdims=True), axis=1, keepdims=True)

    count = total(mask)
    mean = total(mask * adv) / count
    var = total(mask * adv * adv) / count - mean * mean
    white = mask * (adv - mean) * lax.rsqrt(var + WHITEN_EPS)
    for out, z in ((v_ref, values), (ret_ref, mask * (adv + values)), (white_ref, white)):
        mine = z[:ROWS]
        moved = mine
        for piece in range(1, CP):
            moved = jnp.where(cp == piece, pltpu.roll(mine, SEQ - piece * PIECE, 1), moved)
        out[...] = moved[:, :PIECE]


def vmem():
    return pl.BlockSpec(memory_space=pltpu.VMEM)


def smem():
    return pl.BlockSpec(memory_space=pltpu.SMEM)


def hbm():
    return pl.BlockSpec(memory_space=pl.ANY)


def solution(mesh):
    def local_step(x_blk, norm_gain, w_gate, w_up, w_down, final_gain, w_value, b_value, rew_blk, mask_blk):
        rows, piece, model = x_blk.shape
        f32, bf16 = jnp.float32, jnp.bfloat16
        x = x_blk.reshape(TOK, model)
        width = model // SEND_CHUNKS
        slot_shapes = tuple(jax.ShapeDtypeStruct((SLOTS,) + z, bf16) for z in ((model, FC), (model, FC), (FC, model)))
        xs, code, cnt, gm, *slots = pl.pallas_call(
            gather_kernel,
            name='gather_tokens',
            out_shape=(jax.ShapeDtypeStruct((TOK, model), bf16), jax.ShapeDtypeStruct((TOK, SEQ), f32),
                       jax.ShapeDtypeStruct((8, 128), f32), jax.ShapeDtypeStruct((2, DP * ROWS, SEQ), f32)) + slot_shapes,
            in_specs=[hbm()] * 6,
            out_specs=(vmem(),) * 7,
            scratch_shapes=[
                pltpu.VMEM((TOK, model), bf16),
                pltpu.VMEM((rows, piece), jnp.int32), pltpu.VMEM((rows, piece), f32),
                pltpu.VMEM((SEND_CHUNKS, HALF, width), f32), pltpu.VMEM((SEND_CHUNKS, HALF, width), f32),
                pltpu.VMEM((2, ROWS, SEQ), f32), pltpu.VMEM((DP * CP - 1, 2, ROWS, SEQ), f32),
                pltpu.VMEM((2, ROWS, SEQ), f32),
                pltpu.SemaphoreType.DMA((3, SLOTS)), pltpu.SemaphoreType.DMA((3,)),
                pltpu.SemaphoreType.DMA((DP * CP - 1,)), pltpu.SemaphoreType.DMA((DP * CP - 1,)),
                pltpu.SemaphoreType.DMA((SEND_CHUNKS,)), pltpu.SemaphoreType.DMA((SEND_CHUNKS,)),
            ],
            compiler_params=pltpu.CompilerParams(collective_id=0, has_side_effects=True, vmem_limit_bytes=16 << 20),
        )(*(pltpu.with_memory_space_constraint(z, pltpu.HBM) for z in (x, mask_blk, rew_blk, w_gate, w_up, w_down)))
        vals, *_ = pl.pallas_call(
            mlp_kernel,
            name='active_mlp',
            out_shape=(jax.ShapeDtypeStruct((ROWS, SEQ), f32),) + slot_shapes,
            in_specs=[vmem()] * 3 + [hbm()] * 3 + [smem()] + [hbm()] * 3 + [vmem()] * 3,
            out_specs=(vmem(),) * 4,
            input_output_aliases={10: 1, 11: 2, 12: 3},
            scratch_shapes=[
                pltpu.VMEM((1, model), f32), pltpu.VMEM((1, model), f32), pltpu.VMEM((1, model), f32),
                pltpu.VMEM((TOK, model), bf16), pltpu.VMEM((TOK, model), f32), pltpu.VMEM((SIZES[-1], UNIT * FC), bf16),
                pltpu.VMEM((TOK, SEQ), f32),
                pltpu.SemaphoreType.DMA((3,)), pltpu.SemaphoreType.DMA((3, SLOTS)),
            ],
            compiler_params=pltpu.CompilerParams(vmem_limit_bytes=18 << 20),
        )(cnt, xs, code, *(pltpu.with_memory_space_constraint(z.reshape(1, model), pltpu.HBM)
                          for z in (norm_gain, final_gain, w_value)), b_value.reshape(1),
          *(pltpu.with_memory_space_constraint(z, pltpu.HBM) for z in (w_gate, w_up, w_down)), *slots)
        both = pl.pallas_call(
            share_kernel,
            name='share_values',
            out_shape=jax.ShapeDtypeStruct((DP * ROWS, SEQ), f32),
            in_specs=[vmem()],
            out_specs=vmem(),
            scratch_shapes=[
                pltpu.VMEM((DP * CP - 1, ROWS, SEQ), f32),
                pltpu.SemaphoreType.DMA((DP * CP - 1,)), pltpu.SemaphoreType.DMA((DP * CP - 1,)),
            ],
            compiler_params=pltpu.CompilerParams(collective_id=1, has_side_effects=True, vmem_limit_bytes=4 << 20),
        )(vals)
        block = jax.ShapeDtypeStruct((rows, piece), f32)
        return pl.pallas_call(
            gae_kernel,
            name='gae',
            out_shape=(block, block, block),
            in_specs=[vmem(), vmem()],
            out_specs=(vmem(),) * 3,
            compiler_params=pltpu.CompilerParams(vmem_limit_bytes=4 << 20),
        )(both, gm)

    tok_spec = P('dp', 'cp')
    in_specs = (P('dp', 'cp', None), P(None), P(None, None), P(None, None), P(None, None), P(None), P(None), P(),
                tok_spec, tok_spec)
    return jax.shard_map(local_step, mesh=mesh, in_specs=in_specs, out_specs=(tok_spec,) * 3, check_vma=False)
```

```python
import functools
import math

import jax
import jax.numpy as jnp
from jax import lax
from jax.experimental import pallas as pl
from jax.experimental.pallas import tpu as pltpu
from jax.sharding import PartitionSpec as P

NORM_EPS = 1e-6
WHITEN_EPS = 1e-8
DISCOUNT = 1.0
GAE_LAMBDA = 0.995
MESH = pl.DeviceIdType.MESH

ROWS, PIECE, CP, DP = 16, 32, 4, 2
SEQ = PIECE * CP
TOK = ROWS * PIECE
HALF = TOK // 2
SEND_CHUNKS = 4
FC = 256
SLOTS = 12
EARLY = 6
UNIT = 3
SIZES = tuple(range(192, 321, 16))
BLOCK = 64


def iota(shape, dim):
    return lax.broadcasted_iota(jnp.int32, shape, dim)


def everyone(dp, cp):
    for step in range(1, DP * CP):
        yield lax.rem(dp + step // CP, DP), lax.rem(cp + step % CP, CP)


def token_row(placed):
    spread = (lax.rem(iota((SEQ, TOK), 0), PIECE) == lax.rem(iota((SEQ, TOK), 1), PIECE)).astype(jnp.bfloat16)
    by_row = jnp.dot(placed.astype(jnp.bfloat16), spread, preferred_element_type=jnp.float32)
    own = iota((ROWS, TOK), 0) == iota((ROWS, TOK), 1) // PIECE
    return jnp.sum(jnp.where(own, by_row, 0.0), axis=0, keepdims=True)


def token_rank(row):
    upper = (iota((TOK, TOK), 0) <= iota((TOK, TOK), 1)).astype(jnp.bfloat16)
    upto = jnp.dot(jnp.broadcast_to(row, (8, TOK)).astype(jnp.bfloat16), upper, preferred_element_type=jnp.float32)[:1]
    return jnp.where(row > 0.0, upto - 1.0, -1.0)


def weight_copies(chunk, slot, hbm_refs, slots, sems):
    at = pl.ds(pl.multiple_of(chunk * FC, FC), FC)
    return [pltpu.make_async_copy(hbm_refs[w].at[at, :] if w == 2 else hbm_refs[w].at[:, at], slots[w].at[slot],
                                  sems.at[w, slot]) for w in range(3)]


def gather_kernel(x_hbm, mask_hbm, rew_hbm, gain_hbm, final_hbm, wv_hbm, wg_hbm, wu_hbm, wd_hbm,
                  xs_ref, code_ref, cnt_ref, gm_ref, gain_ref, final_ref, wv_ref, wg_buf, wu_buf, wd_buf,
                  x_v, mask_v, rew_v, sendbuf, recvbuf, pack, packs, place, w_sems, in_sem, pk_send, pk_recv, x_send, x_recv):
    dp, cp = lax.axis_index('dp'), lax.axis_index('cp')
    mate = cp + 1 - 2 * lax.rem(cp, 2)
    loads = [pltpu.make_async_copy(src, dst, in_sem.at[k])
             for k, (src, dst) in enumerate(((mask_hbm, mask_v), (rew_hbm, rew_v), (x_hbm, x_v), (gain_hbm, gain_ref), (final_hbm, final_ref),
                                            (wv_hbm, wv_ref)))]
    for load in loads:
        load.start()
    early = [copy for i in range(EARLY) for copy in
             weight_copies(i, i, (wg_hbm, wu_hbm, wd_hbm), (wg_buf, wu_buf, wd_buf), w_sems)]
    for copy in early:
        copy.start(priority=1)
    barrier = pltpu.get_barrier_semaphore()
    for to in everyone(dp, cp):
        pl.semaphore_signal(barrier, inc=1, device_id=to, device_id_type=MESH)

    loads[0].wait()
    loads[1].wait()
    mask_f = mask_v[...].astype(jnp.float32)
    for half, block in enumerate((mask_f, jnp.where(mask_f > 0.0, rew_v[...], 0.0))):
        place[half] = jnp.zeros((ROWS, SEQ), jnp.float32)
        place[half, :, :PIECE] = block
        base = place[half]
        moved = base
        for piece in range(1, CP):
            moved = jnp.where(cp == piece, pltpu.roll(base, piece * PIECE, 1), moved)
        pack[half] = moved
    row = token_row(pack[0])
    rank = token_rank(row)
    pl.semaphore_wait(barrier, DP * CP - 1)

    me = dp * CP + cp
    shares = []
    for k, to in enumerate(everyone(dp, cp)):
        share = pltpu.make_async_remote_copy(
            src_ref=pack, dst_ref=packs.at[k], send_sem=pk_send.at[k], recv_sem=pk_recv.at[k],
            device_id=to, device_id_type=MESH)
        share.start()
        shares.append(share)

    loads[2].wait()
    send_rank = (2 * iota((HALF, TOK), 0) + 1).astype(jnp.float32)
    pick = (rank == send_rank).astype(jnp.bfloat16)
    width = x_v.shape[1] // SEND_CHUNKS
    moves = []
    for j in range(SEND_CHUNKS):
        cols = slice(j * width, (j + 1) * width)
        sendbuf[j] = jnp.dot(pick, x_v[:, cols], preferred_element_type=jnp.float32)
        move = pltpu.make_async_remote_copy(
            src_ref=sendbuf.at[j], dst_ref=recvbuf.at[j], send_sem=x_send.at[j], recv_sem=x_recv.at[j],
            device_id=(dp, mate), device_id_type=MESH)
        move.start()
        moves.append(move)

    for share in shares:
        share.wait_recv()
    placed = [[pack[half] for half in range(2)]] + [[packs[k, half] for half in range(2)] for k in range(DP * CP - 1)]
    same = [sum(placed[k][half] for k in range(CP)) for half in range(2)]
    other = [sum(placed[k][half] for k in range(CP, 2 * CP)) for half in range(2)]
    for half in range(2):
        gm_ref[half, :ROWS, :] = same[half]
        gm_ref[half, ROWS:, :] = other[half]
    lane = iota((ROWS, SEQ), 1)
    mate_row = token_row(jnp.where(lane // PIECE == mate, same[0], 0.0))
    mate_rank = token_rank(mate_row)
    got = jnp.floor(jnp.sum(mate_row, axis=1, keepdims=True) * 0.5)
    keep = jnp.floor((jnp.sum(row, axis=1, keepdims=True) + 1.0) * 0.5)
    cnt_ref[...] = jnp.broadcast_to(got + keep, (8, 128))

    slot = iota((TOK, TOK), 0).astype(jnp.float32)
    own = jnp.logical_and(rank == 2.0 * (slot - got), slot >= got).astype(jnp.bfloat16)
    theirs = (mate_rank == send_rank).astype(jnp.bfloat16)
    tok, half = iota((TOK, 2 * SEQ), 0), iota((TOK, 2 * SEQ), 1) // SEQ

    def codes(pick, piece):
        parts = jnp.where(half == 0, tok // PIECE, lax.rem(tok, PIECE) + piece * PIECE)
        parts = jnp.dot(pick, parts.astype(jnp.float32).astype(jnp.bfloat16), preferred_element_type=jnp.float32)
        return parts[:, :SEQ] * SEQ + parts[:, SEQ:]

    code = codes(own, cp)
    code_ref[...] = code
    code_ref[:HALF, :] = code[:HALF] + codes(theirs, mate)
    came = iota((HALF, width), 0).astype(jnp.float32) < got
    for j in range(SEND_CHUNKS):
        cols = slice(j * width, (j + 1) * width)
        xs_ref[:, cols] = jnp.dot(own, x_v[:, cols], preferred_element_type=jnp.float32).astype(jnp.bfloat16)
    for j in range(SEND_CHUNKS):
        cols = slice(j * width, (j + 1) * width)
        moves[j].wait_recv()
        xs_ref[:HALF, cols] = jnp.where(came, recvbuf[j], xs_ref[:HALF, cols].astype(jnp.float32)).astype(jnp.bfloat16)
    for share in shares:
        share.wait_send()
    for move in moves:
        move.wait_send()
    for copy in loads[3:] + early:
        copy.wait()


def mlp_kernel(cnt_ref, xs_ref, code_ref, gain_ref, final_ref, wv_ref, bv_ref, wg_hbm, wu_hbm, wd_hbm,
               wg_in, wu_in, wd_in, out_ref, wg_buf, wu_buf, wd_buf,
               xn, acc, inner, sems):
    chunks = wd_hbm.shape[0] // FC
    model = xs_ref.shape[1]
    quarters = [slice(q * model // 4, (q + 1) * model // 4) for q in range(4)]

    def copies(i):
        return weight_copies(lax.rem(i, chunks), lax.rem(i, SLOTS), (wg_hbm, wu_hbm, wd_hbm), (wg_buf, wu_buf, wd_buf), sems)

    for i in range(EARLY, SLOTS):
        for copy in copies(i):
            copy.start(priority=1)
    count = jnp.max(cnt_ref[...]).astype(jnp.int32)
    passes = jnp.where(count > SIZES[-1], 2, 1)
    per = jnp.where(count > SIZES[-1], (count + 63) // 64 * 32, count)
    blocks = (count + BLOCK - 1) // BLOCK

    def wait(i):
        @pl.when(i >= EARLY)
        def _():
            for copy in copies(i):
                copy.wait()

    def refill(i):
        @pl.when(i + SLOTS < passes * chunks)
        def _():
            for copy in copies(i + SLOTS):
                copy.start(priority=1)

    def norm(b, _):
        rows = pl.ds(pl.multiple_of(b * BLOCK, BLOCK), BLOCK)
        x = xs_ref[rows, :].astype(jnp.float32)
        scale = lax.rsqrt(jnp.mean(x * x, axis=-1, keepdims=True) + NORM_EPS)
        xn[rows, :] = (x * scale * gain_ref[...]).astype(jnp.bfloat16)
        acc[rows, :] = jnp.zeros((BLOCK, model), jnp.float32)
        return 0

    lax.fori_loop(0, blocks, norm, 0)

    def run(size, p):
        rows = pl.ds(pl.multiple_of(p * per, 32), size)
        begin = p * chunks

        def inside(i, where):
            slot = lax.rem(i, SLOTS)
            gate = jnp.dot(xn[rows, :], wg_buf[slot], preferred_element_type=jnp.float32)
            up = jnp.dot(xn[rows, :], wu_buf[slot], preferred_element_type=jnp.float32)
            inner[:size, where * FC:(where + 1) * FC] = (jax.nn.silu(gate) * up).astype(jnp.bfloat16)

        def down(i, where, cols):
            return jnp.dot(inner[:size, where * FC:(where + 1) * FC], wd_buf[lax.rem(i, SLOTS), :, cols],
                           preferred_element_type=jnp.float32)

        def body(j, _):
            unit = [begin + UNIT * j + k for k in range(UNIT)]
            for i in unit:
                wait(i)
            @pl.when(j > 0)
            def _():
                for k in range(UNIT):
                    refill(unit[0] - UNIT + k)
            for k, i in enumerate(unit):
                inside(i, k)
            for cols in quarters:
                acc[rows, cols] += sum(down(i, k, cols) for k, i in enumerate(unit))
            return 0

        lax.fori_loop(0, chunks // UNIT, body, 0)
        last = begin + chunks - 1
        wait(last)
        for k in range(UNIT):
            refill(last - UNIT + k)
        inside(last, 0)
        for cols in quarters:
            acc[rows, cols] += down(last, 0, cols)
        refill(last)

    def one_pass(p, _):
        for k, size in enumerate(SIZES):
            above = SIZES[k - 1] if k else -1
            @pl.when(jnp.logical_and(per > above, per <= size))
            def _():
                run(size, p)
        return 0

    lax.fori_loop(0, passes, one_pass, 0)

    head_vec = final_ref[...] * wv_ref[...]
    here = iota((1, SEQ), 1).astype(jnp.float32)

    def head(b, placed):
        rows = pl.ds(pl.multiple_of(b * BLOCK, BLOCK), BLOCK)
        h = xs_ref[rows, :].astype(jnp.float32) + acc[rows, :]
        scale = lax.rsqrt(jnp.mean(h * h, axis=-1, keepdims=True) + NORM_EPS)
        val = jnp.sum(h * head_vec, axis=-1, keepdims=True) * scale + bv_ref[0]
        val = jnp.where(iota((BLOCK, 1), 0) + b * BLOCK < count, val, 0.0)
        code = code_ref[rows, :]
        for r in range(ROWS):
            mine = jnp.sum(jnp.where(code == here + r * SEQ, val, 0.0), axis=0, keepdims=True)
            placed = placed + jnp.where(iota((ROWS, SEQ), 0) == r, mine, 0.0)
        return placed

    out_ref[...] = lax.fori_loop(0, blocks, head, jnp.zeros((ROWS, SEQ), jnp.float32))


def share_kernel(vals_ref, all_ref, came, send, recv):
    dp, cp = lax.axis_index('dp'), lax.axis_index('cp')
    barrier = pltpu.get_barrier_semaphore()
    for to in everyone(dp, cp):
        pl.semaphore_signal(barrier, inc=1, device_id=to, device_id_type=MESH)
    pl.semaphore_wait(barrier, DP * CP - 1)
    shares = []
    for k, to in enumerate(everyone(dp, cp)):
        share = pltpu.make_async_remote_copy(
            src_ref=vals_ref, dst_ref=came.at[k], send_sem=send.at[k], recv_sem=recv.at[k],
            device_id=to, device_id_type=MESH)
        share.start()
        shares.append(share)
    for share in shares:
        share.wait_recv()
    all_ref[:ROWS, :] = vals_ref[...] + came[0] + came[1] + came[2]
    all_ref[ROWS:, :] = came[3] + came[4] + came[5] + came[6]
    for share in shares:
        share.wait_send()


def gae_kernel(vals_ref, gm_ref, v_ref, ret_ref, white_ref):
    cp = lax.axis_index('cp')
    values = vals_ref[...]
    mask, rew = gm_ref[0], gm_ref[1]
    lane = iota((2 * ROWS, SEQ), 1)

    def ahead(z, step):
        return jnp.where(lane < SEQ - step, pltpu.roll(z, SEQ - step, 1), 0.0)

    adv = rew + DISCOUNT * ahead(values, 1) - values
    step = 1
    while step < SEQ:
        adv = adv + math.pow(DISCOUNT * GAE_LAMBDA, step) * ahead(adv, step)
        step *= 2

    def total(z):
        return jnp.sum(jnp.sum(z, axis=0, keepdims=True), axis=1, keepdims=True)

    count = total(mask)
    mean = total(mask * adv) / count
    var = total(mask * adv * adv) / count - mean * mean
    white = mask * (adv - mean) * lax.rsqrt(var + WHITEN_EPS)
    for out, z in ((v_ref, values), (ret_ref, mask * (adv + values)), (white_ref, white)):
        mine = z[:ROWS]
        moved = mine
        for piece in range(1, CP):
            moved = jnp.where(cp == piece, pltpu.roll(mine, SEQ - piece * PIECE, 1), moved)
        out[...] = moved[:, :PIECE]


def vmem():
    return pl.BlockSpec(memory_space=pltpu.VMEM)


def smem():
    return pl.BlockSpec(memory_space=pltpu.SMEM)


def hbm():
    return pl.BlockSpec(memory_space=pl.ANY)


def solution(mesh):
    def local_step(x_blk, norm_gain, w_gate, w_up, w_down, final_gain, w_value, b_value, rew_blk, mask_blk):
        rows, piece, model = x_blk.shape
        f32, bf16 = jnp.float32, jnp.bfloat16
        x = x_blk.reshape(TOK, model)
        width = model // SEND_CHUNKS
        slot_shapes = tuple(jax.ShapeDtypeStruct((SLOTS,) + z, bf16) for z in ((model, FC), (model, FC), (FC, model)))
        vec = jax.ShapeDtypeStruct((1, model), f32)
        xs, code, cnt, gm, gain, final, wv, *slots = pl.pallas_call(
            gather_kernel,
            name='gather_tokens',
            out_shape=(jax.ShapeDtypeStruct((TOK, model), bf16), jax.ShapeDtypeStruct((TOK, SEQ), f32),
                       jax.ShapeDtypeStruct((8, 128), f32), jax.ShapeDtypeStruct((2, DP * ROWS, SEQ), f32), vec, vec, vec) + slot_shapes,
            in_specs=[hbm()] * 9,
            out_specs=(vmem(),) * 10,
            scratch_shapes=[
                pltpu.VMEM((TOK, model), bf16),
                pltpu.VMEM((rows, piece), jnp.int32), pltpu.VMEM((rows, piece), f32),
                pltpu.VMEM((SEND_CHUNKS, HALF, width), f32), pltpu.VMEM((SEND_CHUNKS, HALF, width), f32),
                pltpu.VMEM((2, ROWS, SEQ), f32), pltpu.VMEM((DP * CP - 1, 2, ROWS, SEQ), f32),
                pltpu.VMEM((2, ROWS, SEQ), f32),
                pltpu.SemaphoreType.DMA((3, SLOTS)), pltpu.SemaphoreType.DMA((6,)),
                pltpu.SemaphoreType.DMA((DP * CP - 1,)), pltpu.SemaphoreType.DMA((DP * CP - 1,)),
                pltpu.SemaphoreType.DMA((SEND_CHUNKS,)), pltpu.SemaphoreType.DMA((SEND_CHUNKS,)),
            ],
            compiler_params=pltpu.CompilerParams(collective_id=0, has_side_effects=True, vmem_limit_bytes=11 << 20),
        )(*(pltpu.with_memory_space_constraint(z, pltpu.HBM) for z in (x, mask_blk, rew_blk, norm_gain.reshape(1, model), final_gain.reshape(1, model),
                      w_value.reshape(1, model), w_gate, w_up, w_down)))
        vals, *_ = pl.pallas_call(
            mlp_kernel,
            name='active_mlp',
            out_shape=(jax.ShapeDtypeStruct((ROWS, SEQ), f32),) + slot_shapes,
            in_specs=[vmem()] * 6 + [smem()] + [hbm()] * 3 + [vmem()] * 3,
            out_specs=(vmem(),) * 4,
            input_output_aliases={10: 1, 11: 2, 12: 3},
            scratch_shapes=[
                pltpu.VMEM((TOK, model), bf16), pltpu.VMEM((TOK, model), f32), pltpu.VMEM((SIZES[-1], UNIT * FC), bf16),
                pltpu.SemaphoreType.DMA((3, SLOTS)),
            ],
            compiler_params=pltpu.CompilerParams(vmem_limit_bytes=12 << 20),
        )(cnt, xs, code, gain, final, wv, b_value.reshape(1),
          *(pltpu.with_memory_space_constraint(z, pltpu.HBM) for z in (w_gate, w_up, w_down)), *slots)
        both = pl.pallas_call(
            share_kernel,
            name='share_values',
            out_shape=jax.ShapeDtypeStruct((DP * ROWS, SEQ), f32),
            in_specs=[vmem()],
            out_specs=vmem(),
            scratch_shapes=[
                pltpu.VMEM((DP * CP - 1, ROWS, SEQ), f32),
                pltpu.SemaphoreType.DMA((DP * CP - 1,)), pltpu.SemaphoreType.DMA((DP * CP - 1,)),
            ],
            compiler_params=pltpu.CompilerParams(collective_id=1, has_side_effects=True, vmem_limit_bytes=4 << 20),
        )(vals)
        block = jax.ShapeDtypeStruct((rows, piece), f32)
        return pl.pallas_call(
            gae_kernel,
            name='gae',
            out_shape=(block, block, block),
            in_specs=[vmem(), vmem()],
            out_specs=(vmem(),) * 3,
            compiler_params=pltpu.CompilerParams(vmem_limit_bytes=4 << 20),
        )(both, gm)

    tok_spec = P('dp', 'cp')
    in_specs = (P('dp', 'cp', None), P(None), P(None, None), P(None, None), P(None, None), P(None), P(None), P(),
                tok_spec, tok_spec)
    return jax.shard_map(local_step, mesh=mesh, in_specs=in_specs, out_specs=(tok_spec,) * 3, check_vma=False)
```

```python
import functools
import math

import jax
import jax.numpy as jnp
from jax import lax
from jax.experimental import pallas as pl
from jax.experimental.pallas import tpu as pltpu
from jax.sharding import PartitionSpec as P

NORM_EPS = 1e-6
WHITEN_EPS = 1e-8
DISCOUNT = 1.0
GAE_LAMBDA = 0.995
MESH = pl.DeviceIdType.MESH

ROWS, PIECE, CP, DP = 16, 32, 4, 2
SEQ = PIECE * CP
TOK = ROWS * PIECE
WINDOW = 192
SEND_CHUNKS = 4
FC = 256
SLOTS = 12
EARLY = 5
UNIT = 3
SIZES = tuple(range(192, 321, 16))
BLOCK = 64


def iota(shape, dim):
    return lax.broadcasted_iota(jnp.int32, shape, dim)


def everyone(dp, cp):
    for step in range(1, DP * CP):
        yield lax.rem(dp + step // CP, DP), lax.rem(cp + step % CP, CP)


def token_row(placed):
    spread = (lax.rem(iota((SEQ, TOK), 0), PIECE) == lax.rem(iota((SEQ, TOK), 1), PIECE)).astype(jnp.bfloat16)
    by_row = jnp.dot(placed.astype(jnp.bfloat16), spread, preferred_element_type=jnp.float32)
    own = iota((ROWS, TOK), 0) == iota((ROWS, TOK), 1) // PIECE
    return jnp.sum(jnp.where(own, by_row, 0.0), axis=0, keepdims=True)


def token_rank(row):
    upper = (iota((TOK, TOK), 0) <= iota((TOK, TOK), 1)).astype(jnp.bfloat16)
    upto = jnp.dot(jnp.broadcast_to(row, (8, TOK)).astype(jnp.bfloat16), upper, preferred_element_type=jnp.float32)[:1]
    return jnp.where(row > 0.0, upto - 1.0, -1.0)


def weight_copies(chunk, slot, hbm_refs, slots, sems):
    at = pl.ds(pl.multiple_of(chunk * FC, FC), FC)
    return [pltpu.make_async_copy(hbm_refs[w].at[at, :] if w == 2 else hbm_refs[w].at[:, at], slots[w].at[slot],
                                  sems.at[w, slot]) for w in range(3)]


def gather_kernel(x_hbm, mask_hbm, rew_hbm, gain_hbm, final_hbm, wv_hbm, wg_hbm, wu_hbm, wd_hbm,
                  xs_ref, code_ref, cnt_ref, gm_ref, gain_ref, final_ref, wv_ref, wg_buf, wu_buf, wd_buf,
                  x_v, mask_v, rew_v, sendbuf, recvbuf, pack, packs, mate_pack, place, w_sems, in_sem, pk_send, pk_recv, mate_send, mate_recv, x_send, x_recv):
    dp, cp = lax.axis_index('dp'), lax.axis_index('cp')
    mate = cp + 1 - 2 * lax.rem(cp, 2)
    loads = [pltpu.make_async_copy(src, dst, in_sem.at[k])
             for k, (src, dst) in enumerate(((mask_hbm, mask_v), (rew_hbm, rew_v), (x_hbm, x_v), (gain_hbm, gain_ref), (final_hbm, final_ref),
                                            (wv_hbm, wv_ref)))]
    for load in loads:
        load.start()
    early = [copy for i in range(EARLY) for copy in
             weight_copies(i, i, (wg_hbm, wu_hbm, wd_hbm), (wg_buf, wu_buf, wd_buf), w_sems)]
    for copy in early:
        copy.start(priority=1)
    barrier = pltpu.get_barrier_semaphore()
    for to in everyone(dp, cp):
        pl.semaphore_signal(barrier, inc=1, device_id=to, device_id_type=MESH)

    loads[0].wait()
    loads[1].wait()
    mask_f = mask_v[...].astype(jnp.float32)
    for half, block in enumerate((mask_f, jnp.where(mask_f > 0.0, rew_v[...], 0.0))):
        place[half] = jnp.zeros((ROWS, SEQ), jnp.float32)
        place[half, :, :PIECE] = block
        base = place[half]
        moved = base
        for piece in range(1, CP):
            moved = jnp.where(cp == piece, pltpu.roll(base, piece * PIECE, 1), moved)
        pack[half] = moved
    row = token_row(pack[0])
    rank = token_rank(row)
    pl.semaphore_wait(barrier, DP * CP - 1)

    first = pltpu.make_async_remote_copy(
        src_ref=pack, dst_ref=mate_pack, send_sem=mate_send, recv_sem=mate_recv,
        device_id=(dp, mate), device_id_type=MESH)
    first.start()
    shares = []
    for k, to in enumerate(everyone(dp, cp)):
        share = pltpu.make_async_remote_copy(
            src_ref=pack, dst_ref=packs.at[k], send_sem=pk_send.at[k], recv_sem=pk_recv.at[k],
            device_id=to, device_id_type=MESH)
        share.start()
        shares.append(share)

    loads[2].wait()
    send_rank = (2 * iota((WINDOW, TOK), 0) + 1).astype(jnp.float32)
    pick = (rank == send_rank).astype(jnp.bfloat16)
    width = x_v.shape[1] // SEND_CHUNKS
    moves = []
    for j in range(SEND_CHUNKS):
        cols = slice(j * width, (j + 1) * width)
        sendbuf[j] = jnp.dot(pick, x_v[:, cols], preferred_element_type=jnp.float32)
        move = pltpu.make_async_remote_copy(
            src_ref=sendbuf.at[j], dst_ref=recvbuf.at[j], send_sem=x_send.at[j], recv_sem=x_recv.at[j],
            device_id=(dp, mate), device_id_type=MESH)
        move.start()
        moves.append(move)

    first.wait_recv()
    mate_row = token_row(mate_pack[0])
    mate_rank = token_rank(mate_row)
    total = jnp.sum(row, axis=1, keepdims=True)
    gone = jnp.minimum(jnp.floor(total * 0.5), WINDOW)
    got = jnp.minimum(jnp.floor(jnp.sum(mate_row, axis=1, keepdims=True) * 0.5), WINDOW)
    cnt_ref[...] = jnp.broadcast_to(got + total - gone, (8, 128))

    even = rank == 2.0 * jnp.floor(rank * 0.5)
    kept = jnp.where(rank >= 2.0 * WINDOW, rank - WINDOW, jnp.where(even, rank * 0.5, -1.0))
    slot = iota((TOK, TOK), 0).astype(jnp.float32)
    own = jnp.logical_and(kept == slot - got, slot >= got).astype(jnp.bfloat16)
    theirs = (mate_rank == send_rank).astype(jnp.bfloat16)
    tok, half = iota((TOK, 2 * SEQ), 0), iota((TOK, 2 * SEQ), 1) // SEQ

    def codes(pick, piece):
        parts = jnp.where(half == 0, tok // PIECE, lax.rem(tok, PIECE) + piece * PIECE)
        parts = jnp.dot(pick, parts.astype(jnp.float32).astype(jnp.bfloat16), preferred_element_type=jnp.float32)
        return parts[:, :SEQ] * SEQ + parts[:, SEQ:]

    code = codes(own, cp)
    code_ref[...] = code
    code_ref[:WINDOW, :] = code[:WINDOW] + codes(theirs, mate)
    came = iota((WINDOW, width), 0).astype(jnp.float32) < got
    for j in range(SEND_CHUNKS):
        cols = slice(j * width, (j + 1) * width)
        xs_ref[:, cols] = jnp.dot(own, x_v[:, cols], preferred_element_type=jnp.float32).astype(jnp.bfloat16)
    for share in shares:
        share.wait_recv()
    placed = [[pack[half] for half in range(2)]] + [[packs[k, half] for half in range(2)] for k in range(DP * CP - 1)]
    same = [sum(placed[k][half] for k in range(CP)) for half in range(2)]
    other = [sum(placed[k][half] for k in range(CP, 2 * CP)) for half in range(2)]
    for half in range(2):
        gm_ref[half, :ROWS, :] = same[half]
        gm_ref[half, ROWS:, :] = other[half]
    for j in range(SEND_CHUNKS):
        cols = slice(j * width, (j + 1) * width)
        moves[j].wait_recv()
        xs_ref[:WINDOW, cols] = jnp.where(came, recvbuf[j], xs_ref[:WINDOW, cols].astype(jnp.float32)).astype(jnp.bfloat16)
    first.wait_send()
    for share in shares:
        share.wait_send()
    for move in moves:
        move.wait_send()
    for copy in loads[3:] + early:
        copy.wait()


def mlp_kernel(cnt_ref, xs_ref, code_ref, gain_ref, final_ref, wv_ref, bv_ref, wg_hbm, wu_hbm, wd_hbm,
               wg_in, wu_in, wd_in, out_ref, wg_buf, wu_buf, wd_buf,
               xn, acc, inner, sems):
    chunks = wd_hbm.shape[0] // FC
    model = xs_ref.shape[1]
    quarters = [slice(q * model // 4, (q + 1) * model // 4) for q in range(4)]

    def copies(i):
        return weight_copies(lax.rem(i, chunks), lax.rem(i, SLOTS), (wg_hbm, wu_hbm, wd_hbm), (wg_buf, wu_buf, wd_buf), sems)

    for i in range(EARLY, SLOTS):
        for copy in copies(i):
            copy.start(priority=1)
    count = jnp.max(cnt_ref[...]).astype(jnp.int32)
    passes = jnp.where(count > SIZES[-1], 2, 1)
    per = jnp.where(count > SIZES[-1], (count + 63) // 64 * 32, count)
    blocks = (count + BLOCK - 1) // BLOCK

    def wait(i):
        @pl.when(i >= EARLY)
        def _():
            for copy in copies(i):
                copy.wait()

    def refill(i):
        @pl.when(i + SLOTS < passes * chunks)
        def _():
            for copy in copies(i + SLOTS):
                copy.start(priority=1)

    def norm(b, _):
        rows = pl.ds(pl.multiple_of(b * BLOCK, BLOCK), BLOCK)
        x = xs_ref[rows, :].astype(jnp.float32)
        scale = lax.rsqrt(jnp.mean(x * x, axis=-1, keepdims=True) + NORM_EPS)
        xn[rows, :] = (x * scale * gain_ref[...]).astype(jnp.bfloat16)
        acc[rows, :] = jnp.zeros((BLOCK, model), jnp.float32)
        return 0

    lax.fori_loop(0, blocks, norm, 0)

    def run(size, p):
        rows = pl.ds(pl.multiple_of(p * per, 32), size)
        begin = p * chunks

        def inside(i, where):
            slot = lax.rem(i, SLOTS)
            gate = jnp.dot(xn[rows, :], wg_buf[slot], preferred_element_type=jnp.float32)
            up = jnp.dot(xn[rows, :], wu_buf[slot], preferred_element_type=jnp.float32)
            inner[:size, where * FC:(where + 1) * FC] = (jax.nn.silu(gate) * up).astype(jnp.bfloat16)

        def down(i, where, cols):
            return jnp.dot(inner[:size, where * FC:(where + 1) * FC], wd_buf[lax.rem(i, SLOTS), :, cols],
                           preferred_element_type=jnp.float32)

        def body(j, _):
            unit = [begin + UNIT * j + k for k in range(UNIT)]
            for i in unit:
                wait(i)
            @pl.when(j > 0)
            def _():
                for k in range(UNIT):
                    refill(unit[0] - UNIT + k)
            for k, i in enumerate(unit):
                inside(i, k)
            for cols in quarters:
                acc[rows, cols] += sum(down(i, k, cols) for k, i in enumerate(unit))
            return 0

        lax.fori_loop(0, chunks // UNIT, body, 0)
        last = begin + chunks - 1
        wait(last)
        for k in range(UNIT):
            refill(last - UNIT + k)
        inside(last, 0)
        for cols in quarters:
            acc[rows, cols] += down(last, 0, cols)
        refill(last)

    def one_pass(p, _):
        for k, size in enumerate(SIZES):
            above = SIZES[k - 1] if k else -1
            @pl.when(jnp.logical_and(per > above, per <= size))
            def _():
                run(size, p)
        return 0

    lax.fori_loop(0, passes, one_pass, 0)

    head_vec = final_ref[...] * wv_ref[...]
    here = iota((1, SEQ), 1).astype(jnp.float32)

    def head(b, placed):
        rows = pl.ds(pl.multiple_of(b * BLOCK, BLOCK), BLOCK)
        h = xs_ref[rows, :].astype(jnp.float32) + acc[rows, :]
        scale = lax.rsqrt(jnp.mean(h * h, axis=-1, keepdims=True) + NORM_EPS)
        val = jnp.sum(h * head_vec, axis=-1, keepdims=True) * scale + bv_ref[0]
        val = jnp.where(iota((BLOCK, 1), 0) + b * BLOCK < count, val, 0.0)
        code = code_ref[rows, :]
        for r in range(ROWS):
            mine = jnp.sum(jnp.where(code == here + r * SEQ, val, 0.0), axis=0, keepdims=True)
            placed = placed + jnp.where(iota((ROWS, SEQ), 0) == r, mine, 0.0)
        return placed

    out_ref[...] = lax.fori_loop(0, blocks, head, jnp.zeros((ROWS, SEQ), jnp.float32))


def share_kernel(vals_ref, all_ref, came, send, recv):
    dp, cp = lax.axis_index('dp'), lax.axis_index('cp')
    barrier = pltpu.get_barrier_semaphore()
    for to in everyone(dp, cp):
        pl.semaphore_signal(barrier, inc=1, device_id=to, device_id_type=MESH)
    pl.semaphore_wait(barrier, DP * CP - 1)
    shares = []
    for k, to in enumerate(everyone(dp, cp)):
        share = pltpu.make_async_remote_copy(
            src_ref=vals_ref, dst_ref=came.at[k], send_sem=send.at[k], recv_sem=recv.at[k],
            device_id=to, device_id_type=MESH)
        share.start()
        shares.append(share)
    for share in shares:
        share.wait_recv()
    all_ref[:ROWS, :] = vals_ref[...] + came[0] + came[1] + came[2]
    all_ref[ROWS:, :] = came[3] + came[4] + came[5] + came[6]
    for share in shares:
        share.wait_send()


def gae_kernel(vals_ref, gm_ref, v_ref, ret_ref, white_ref):
    cp = lax.axis_index('cp')
    values = vals_ref[...]
    mask, rew = gm_ref[0], gm_ref[1]
    lane = iota((2 * ROWS, SEQ), 1)

    def ahead(z, step):
        return jnp.where(lane < SEQ - step, pltpu.roll(z, SEQ - step, 1), 0.0)

    adv = rew + DISCOUNT * ahead(values, 1) - values
    step = 1
    while step < SEQ:
        adv = adv + math.pow(DISCOUNT * GAE_LAMBDA, step) * ahead(adv, step)
        step *= 2

    def total(z):
        return jnp.sum(jnp.sum(z, axis=0, keepdims=True), axis=1, keepdims=True)

    count = total(mask)
    mean = total(mask * adv) / count
    var = total(mask * adv * adv) / count - mean * mean
    white = mask * (adv - mean) * lax.rsqrt(var + WHITEN_EPS)
    for out, z in ((v_ref, values), (ret_ref, mask * (adv + values)), (white_ref, white)):
        mine = z[:ROWS]
        moved = mine
        for piece in range(1, CP):
            moved = jnp.where(cp == piece, pltpu.roll(mine, SEQ - piece * PIECE, 1), moved)
        out[...] = moved[:, :PIECE]


def vmem():
    return pl.BlockSpec(memory_space=pltpu.VMEM)


def smem():
    return pl.BlockSpec(memory_space=pltpu.SMEM)


def hbm():
    return pl.BlockSpec(memory_space=pl.ANY)


def solution(mesh):
    def local_step(x_blk, norm_gain, w_gate, w_up, w_down, final_gain, w_value, b_value, rew_blk, mask_blk):
        rows, piece, model = x_blk.shape
        f32, bf16 = jnp.float32, jnp.bfloat16
        x = x_blk.reshape(TOK, model)
        width = model // SEND_CHUNKS
        slot_shapes = tuple(jax.ShapeDtypeStruct((SLOTS,) + z, bf16) for z in ((model, FC), (model, FC), (FC, model)))
        vec = jax.ShapeDtypeStruct((1, model), f32)
        xs, code, cnt, gm, gain, final, wv, *slots = pl.pallas_call(
            gather_kernel,
            name='gather_tokens',
            out_shape=(jax.ShapeDtypeStruct((TOK, model), bf16), jax.ShapeDtypeStruct((TOK, SEQ), f32),
                       jax.ShapeDtypeStruct((8, 128), f32), jax.ShapeDtypeStruct((2, DP * ROWS, SEQ), f32), vec, vec, vec) + slot_shapes,
            in_specs=[hbm()] * 9,
            out_specs=(vmem(),) * 10,
            scratch_shapes=[
                pltpu.VMEM((TOK, model), bf16),
                pltpu.VMEM((rows, piece), jnp.int32), pltpu.VMEM((rows, piece), f32),
                pltpu.VMEM((SEND_CHUNKS, WINDOW, width), f32), pltpu.VMEM((SEND_CHUNKS, WINDOW, width), f32),
                pltpu.VMEM((2, ROWS, SEQ), f32), pltpu.VMEM((DP * CP - 1, 2, ROWS, SEQ), f32),
                pltpu.VMEM((2, ROWS, SEQ), f32), pltpu.VMEM((2, ROWS, SEQ), f32),
                pltpu.SemaphoreType.DMA((3, SLOTS)), pltpu.SemaphoreType.DMA((6,)),
                pltpu.SemaphoreType.DMA((DP * CP - 1,)), pltpu.SemaphoreType.DMA((DP * CP - 1,)),
                pltpu.SemaphoreType.DMA, pltpu.SemaphoreType.DMA,
                pltpu.SemaphoreType.DMA((SEND_CHUNKS,)), pltpu.SemaphoreType.DMA((SEND_CHUNKS,)),
            ],
            compiler_params=pltpu.CompilerParams(collective_id=0, has_side_effects=True, vmem_limit_bytes=11 << 20),
        )(*(pltpu.with_memory_space_constraint(z, pltpu.HBM) for z in (x, mask_blk, rew_blk, norm_gain.reshape(1, model), final_gain.reshape(1, model),
                      w_value.reshape(1, model), w_gate, w_up, w_down)))
        vals, *_ = pl.pallas_call(
            mlp_kernel,
            name='active_mlp',
            out_shape=(jax.ShapeDtypeStruct((ROWS, SEQ), f32),) + slot_shapes,
            in_specs=[vmem()] * 6 + [smem()] + [hbm()] * 3 + [vmem()] * 3,
            out_specs=(vmem(),) * 4,
            input_output_aliases={10: 1, 11: 2, 12: 3},
            scratch_shapes=[
                pltpu.VMEM((TOK, model), bf16), pltpu.VMEM((TOK, model), f32), pltpu.VMEM((SIZES[-1], UNIT * FC), bf16),
                pltpu.SemaphoreType.DMA((3, SLOTS)),
            ],
            compiler_params=pltpu.CompilerParams(vmem_limit_bytes=12 << 20),
        )(cnt, xs, code, gain, final, wv, b_value.reshape(1),
          *(pltpu.with_memory_space_constraint(z, pltpu.HBM) for z in (w_gate, w_up, w_down)), *slots)
        both = pl.pallas_call(
            share_kernel,
            name='share_values',
            out_shape=jax.ShapeDtypeStruct((DP * ROWS, SEQ), f32),
            in_specs=[vmem()],
            out_specs=vmem(),
            scratch_shapes=[
                pltpu.VMEM((DP * CP - 1, ROWS, SEQ), f32),
                pltpu.SemaphoreType.DMA((DP * CP - 1,)), pltpu.SemaphoreType.DMA((DP * CP - 1,)),
            ],
            compiler_params=pltpu.CompilerParams(collective_id=1, has_side_effects=True, vmem_limit_bytes=4 << 20),
        )(vals)
        block = jax.ShapeDtypeStruct((rows, piece), f32)
        return pl.pallas_call(
            gae_kernel,
            name='gae',
            out_shape=(block, block, block),
            in_specs=[vmem(), vmem()],
            out_specs=(vmem(),) * 3,
            compiler_params=pltpu.CompilerParams(vmem_limit_bytes=4 << 20),
        )(both, gm)

    tok_spec = P('dp', 'cp')
    in_specs = (P('dp', 'cp', None), P(None), P(None, None), P(None, None), P(None, None), P(None), P(None), P(),
                tok_spec, tok_spec)
    return jax.shard_map(local_step, mesh=mesh, in_specs=in_specs, out_specs=(tok_spec,) * 3, check_vma=False)
```

```python
import functools
import math

import jax
import jax.numpy as jnp
from jax import lax
from jax.experimental import pallas as pl
from jax.experimental.pallas import tpu as pltpu
from jax.sharding import PartitionSpec as P

NORM_EPS = 1e-6
WHITEN_EPS = 1e-8
DISCOUNT = 1.0
GAE_LAMBDA = 0.995
MESH = pl.DeviceIdType.MESH

ROWS, PIECE, CP, DP = 16, 32, 4, 2
SEQ = PIECE * CP
TOK = ROWS * PIECE
WINDOW = 192
SEND_CHUNKS = 4
FC = 256
SLOTS = 12
EARLY = 4
UNIT = 3
SIZES = tuple(range(192, 321, 16))
BLOCK = 64


def iota(shape, dim):
    return lax.broadcasted_iota(jnp.int32, shape, dim)


def everyone(dp, cp):
    for step in range(1, DP * CP):
        yield lax.rem(dp + step // CP, DP), lax.rem(cp + step % CP, CP)


def token_row(placed):
    spread = (lax.rem(iota((SEQ, TOK), 0), PIECE) == lax.rem(iota((SEQ, TOK), 1), PIECE)).astype(jnp.bfloat16)
    by_row = jnp.dot(placed.astype(jnp.bfloat16), spread, preferred_element_type=jnp.float32)
    own = iota((ROWS, TOK), 0) == iota((ROWS, TOK), 1) // PIECE
    return jnp.sum(jnp.where(own, by_row, 0.0), axis=0, keepdims=True)


def token_rank(row):
    upper = (iota((TOK, TOK), 0) <= iota((TOK, TOK), 1)).astype(jnp.bfloat16)
    upto = jnp.dot(jnp.broadcast_to(row, (8, TOK)).astype(jnp.bfloat16), upper, preferred_element_type=jnp.float32)[:1]
    return jnp.where(row > 0.0, upto - 1.0, -1.0)


def weight_copies(chunk, slot, hbm_refs, slots, sems):
    at = pl.ds(pl.multiple_of(chunk * FC, FC), FC)
    return [pltpu.make_async_copy(hbm_refs[w].at[at, :] if w == 2 else hbm_refs[w].at[:, at], slots[w].at[slot],
                                  sems.at[w, slot]) for w in range(3)]


def gather_kernel(x_hbm, mask_hbm, rew_hbm, gain_hbm, final_hbm, wv_hbm, wg_hbm, wu_hbm, wd_hbm,
                  xs_ref, code_ref, cnt_ref, gm_ref, gain_ref, final_ref, wv_ref, wg_buf, wu_buf, wd_buf,
                  x_v, mask_v, rew_v, sendbuf, recvbuf, pack, packs, mate_pack, place, w_sems, in_sem, pk_send, pk_recv, mate_send, mate_recv, x_send, x_recv):
    dp, cp = lax.axis_index('dp'), lax.axis_index('cp')
    mate = cp + 1 - 2 * lax.rem(cp, 2)
    loads = [pltpu.make_async_copy(src, dst, in_sem.at[k])
             for k, (src, dst) in enumerate(((mask_hbm, mask_v), (rew_hbm, rew_v), (x_hbm, x_v), (gain_hbm, gain_ref), (final_hbm, final_ref),
                                            (wv_hbm, wv_ref)))]
    for load in loads:
        load.start()
    early = [copy for i in range(EARLY) for copy in
             weight_copies(i, i, (wg_hbm, wu_hbm, wd_hbm), (wg_buf, wu_buf, wd_buf), w_sems)]
    for copy in early:
        copy.start(priority=1)
    barrier = pltpu.get_barrier_semaphore()
    for to in everyone(dp, cp):
        pl.semaphore_signal(barrier, inc=1, device_id=to, device_id_type=MESH)

    loads[0].wait()
    loads[1].wait()
    mask_f = mask_v[...].astype(jnp.float32)
    for half, block in enumerate((mask_f, jnp.where(mask_f > 0.0, rew_v[...], 0.0))):
        place[half] = jnp.zeros((ROWS, SEQ), jnp.float32)
        place[half, :, :PIECE] = block
        base = place[half]
        moved = base
        for piece in range(1, CP):
            moved = jnp.where(cp == piece, pltpu.roll(base, piece * PIECE, 1), moved)
        pack[half] = moved
    row = token_row(pack[0])
    rank = token_rank(row)
    pl.semaphore_wait(barrier, DP * CP - 1)

    first = pltpu.make_async_remote_copy(
        src_ref=pack, dst_ref=mate_pack, send_sem=mate_send, recv_sem=mate_recv,
        device_id=(dp, mate), device_id_type=MESH)
    first.start()
    shares = []
    for k, to in enumerate(everyone(dp, cp)):
        share = pltpu.make_async_remote_copy(
            src_ref=pack, dst_ref=packs.at[k], send_sem=pk_send.at[k], recv_sem=pk_recv.at[k],
            device_id=to, device_id_type=MESH)
        share.start()
        shares.append(share)

    loads[2].wait()
    send_rank = (2 * iota((WINDOW, TOK), 0) + 1).astype(jnp.float32)
    pick = (rank == send_rank).astype(jnp.bfloat16)
    width = x_v.shape[1] // SEND_CHUNKS
    moves = []
    for j in range(SEND_CHUNKS):
        cols = slice(j * width, (j + 1) * width)
        sendbuf[j] = jnp.dot(pick, x_v[:, cols], preferred_element_type=jnp.float32)
        move = pltpu.make_async_remote_copy(
            src_ref=sendbuf.at[j], dst_ref=recvbuf.at[j], send_sem=x_send.at[j], recv_sem=x_recv.at[j],
            device_id=(dp, mate), device_id_type=MESH)
        move.start()
        moves.append(move)

    first.wait_recv()
    mate_row = token_row(mate_pack[0])
    mate_rank = token_rank(mate_row)
    total = jnp.sum(row, axis=1, keepdims=True)
    gone = jnp.minimum(jnp.floor(total * 0.5), WINDOW)
    got = jnp.minimum(jnp.floor(jnp.sum(mate_row, axis=1, keepdims=True) * 0.5), WINDOW)
    cnt_ref[...] = jnp.broadcast_to(got + total - gone, (8, 128))

    even = rank == 2.0 * jnp.floor(rank * 0.5)
    kept = jnp.where(rank >= 2.0 * WINDOW, rank - WINDOW, jnp.where(even, rank * 0.5, -1.0))
    slot = iota((TOK, TOK), 0).astype(jnp.float32)
    own = jnp.logical_and(kept == slot - got, slot >= got).astype(jnp.bfloat16)
    theirs = (mate_rank == send_rank).astype(jnp.bfloat16)
    tok, half = iota((TOK, 2 * SEQ), 0), iota((TOK, 2 * SEQ), 1) // SEQ

    def codes(pick, piece):
        parts = jnp.where(half == 0, tok // PIECE, lax.rem(tok, PIECE) + piece * PIECE)
        parts = jnp.dot(pick, parts.astype(jnp.float32).astype(jnp.bfloat16), preferred_element_type=jnp.float32)
        return parts[:, :SEQ] * SEQ + parts[:, SEQ:]

    code = codes(own, cp)
    code_ref[...] = code
    code_ref[:WINDOW, :] = code[:WINDOW] + codes(theirs, mate)
    came = iota((WINDOW, width), 0).astype(jnp.float32) < got
    for j in range(SEND_CHUNKS):
        cols = slice(j * width, (j + 1) * width)
        xs_ref[:, cols] = jnp.dot(own, x_v[:, cols], preferred_element_type=jnp.float32).astype(jnp.bfloat16)
    for share in shares:
        share.wait_recv()
    placed = [[pack[half] for half in range(2)]] + [[packs[k, half] for half in range(2)] for k in range(DP * CP - 1)]
    same = [sum(placed[k][half] for k in range(CP)) for half in range(2)]
    other = [sum(placed[k][half] for k in range(CP, 2 * CP)) for half in range(2)]
    for half in range(2):
        gm_ref[half, :ROWS, :] = same[half]
        gm_ref[half, ROWS:, :] = other[half]
    for j in range(SEND_CHUNKS):
        cols = slice(j * width, (j + 1) * width)
        moves[j].wait_recv()
        xs_ref[:WINDOW, cols] = jnp.where(came, recvbuf[j], xs_ref[:WINDOW, cols].astype(jnp.float32)).astype(jnp.bfloat16)
    first.wait_send()
    for share in shares:
        share.wait_send()
    for move in moves:
        move.wait_send()
    for copy in loads[3:] + early:
        copy.wait()


def mlp_kernel(cnt_ref, xs_ref, code_ref, gain_ref, final_ref, wv_ref, bv_ref, wg_hbm, wu_hbm, wd_hbm,
               wg_in, wu_in, wd_in, out_ref, wg_buf, wu_buf, wd_buf,
               xn, acc, inner, sems):
    chunks = wd_hbm.shape[0] // FC
    model = xs_ref.shape[1]
    quarters = [slice(q * model // 4, (q + 1) * model // 4) for q in range(4)]

    def copies(i):
        return weight_copies(lax.rem(i, chunks), lax.rem(i, SLOTS), (wg_hbm, wu_hbm, wd_hbm), (wg_buf, wu_buf, wd_buf), sems)

    for i in range(EARLY, SLOTS):
        for copy in copies(i):
            copy.start(priority=1)
    count = jnp.max(cnt_ref[...]).astype(jnp.int32)
    passes = jnp.where(count > SIZES[-1], 2, 1)
    per = jnp.where(count > SIZES[-1], (count + 63) // 64 * 32, count)
    blocks = (count + BLOCK - 1) // BLOCK

    def wait(i):
        @pl.when(i >= EARLY)
        def _():
            for copy in copies(i):
                copy.wait()

    def refill(i):
        @pl.when(i + SLOTS < passes * chunks)
        def _():
            for copy in copies(i + SLOTS):
                copy.start(priority=1)

    def norm(b, _):
        rows = pl.ds(pl.multiple_of(b * BLOCK, BLOCK), BLOCK)
        x = xs_ref[rows, :].astype(jnp.float32)
        scale = lax.rsqrt(jnp.mean(x * x, axis=-1, keepdims=True) + NORM_EPS)
        xn[rows, :] = (x * scale * gain_ref[...]).astype(jnp.bfloat16)
        acc[rows, :] = jnp.zeros((BLOCK, model), jnp.float32)
        return 0

    lax.fori_loop(0, blocks, norm, 0)

    def run(size, p):
        rows = pl.ds(pl.multiple_of(p * per, 32), size)
        begin = p * chunks

        def inside(i, where):
            slot = lax.rem(i, SLOTS)
            gate = jnp.dot(xn[rows, :], wg_buf[slot], preferred_element_type=jnp.float32)
            up = jnp.dot(xn[rows, :], wu_buf[slot], preferred_element_type=jnp.float32)
            inner[:size, where * FC:(where + 1) * FC] = (jax.nn.silu(gate) * up).astype(jnp.bfloat16)

        def down(i, where, cols):
            return jnp.dot(inner[:size, where * FC:(where + 1) * FC], wd_buf[lax.rem(i, SLOTS), :, cols],
                           preferred_element_type=jnp.float32)

        def body(j, _):
            unit = [begin + UNIT * j + k for k in range(UNIT)]
            for i in unit:
                wait(i)
            @pl.when(j > 0)
            def _():
                for k in range(UNIT):
                    refill(unit[0] - UNIT + k)
            for k, i in enumerate(unit):
                inside(i, k)
            for cols in quarters:
                acc[rows, cols] += sum(down(i, k, cols) for k, i in enumerate(unit))
            return 0

        lax.fori_loop(0, chunks // UNIT, body, 0)
        last = begin + chunks - 1
        wait(last)
        for k in range(UNIT):
            refill(last - UNIT + k)
        inside(last, 0)
        for cols in quarters:
            acc[rows, cols] += down(last, 0, cols)
        refill(last)

    def one_pass(p, _):
        for k, size in enumerate(SIZES):
            above = SIZES[k - 1] if k else -1
            @pl.when(jnp.logical_and(per > above, per <= size))
            def _():
                run(size, p)
        return 0

    lax.fori_loop(0, passes, one_pass, 0)

    head_vec = final_ref[...] * wv_ref[...]
    here = iota((1, SEQ), 1).astype(jnp.float32)

    def head(b, placed):
        rows = pl.ds(pl.multiple_of(b * BLOCK, BLOCK), BLOCK)
        h = xs_ref[rows, :].astype(jnp.float32) + acc[rows, :]
        scale = lax.rsqrt(jnp.mean(h * h, axis=-1, keepdims=True) + NORM_EPS)
        val = jnp.sum(h * head_vec, axis=-1, keepdims=True) * scale + bv_ref[0]
        val = jnp.where(iota((BLOCK, 1), 0) + b * BLOCK < count, val, 0.0)
        code = code_ref[rows, :]
        for r in range(ROWS):
            mine = jnp.sum(jnp.where(code == here + r * SEQ, val, 0.0), axis=0, keepdims=True)
            placed = placed + jnp.where(iota((ROWS, SEQ), 0) == r, mine, 0.0)
        return placed

    out_ref[...] = lax.fori_loop(0, blocks, head, jnp.zeros((ROWS, SEQ), jnp.float32))


def share_kernel(vals_ref, all_ref, came, send, recv):
    dp, cp = lax.axis_index('dp'), lax.axis_index('cp')
    barrier = pltpu.get_barrier_semaphore()
    for to in everyone(dp, cp):
        pl.semaphore_signal(barrier, inc=1, device_id=to, device_id_type=MESH)
    pl.semaphore_wait(barrier, DP * CP - 1)
    shares = []
    for k, to in enumerate(everyone(dp, cp)):
        share = pltpu.make_async_remote_copy(
            src_ref=vals_ref, dst_ref=came.at[k], send_sem=send.at[k], recv_sem=recv.at[k],
            device_id=to, device_id_type=MESH)
        share.start()
        shares.append(share)
    for share in shares:
        share.wait_recv()
    all_ref[:ROWS, :] = vals_ref[...] + came[0] + came[1] + came[2]
    all_ref[ROWS:, :] = came[3] + came[4] + came[5] + came[6]
    for share in shares:
        share.wait_send()


def gae_kernel(vals_ref, gm_ref, v_ref, ret_ref, white_ref):
    cp = lax.axis_index('cp')
    values = vals_ref[...]
    mask, rew = gm_ref[0], gm_ref[1]
    lane = iota((2 * ROWS, SEQ), 1)

    def ahead(z, step):
        return jnp.where(lane < SEQ - step, pltpu.roll(z, SEQ - step, 1), 0.0)

    adv = rew + DISCOUNT * ahead(values, 1) - values
    step = 1
    while step < SEQ:
        adv = adv + math.pow(DISCOUNT * GAE_LAMBDA, step) * ahead(adv, step)
        step *= 2

    def total(z):
        return jnp.sum(jnp.sum(z, axis=0, keepdims=True), axis=1, keepdims=True)

    count = total(mask)
    mean = total(mask * adv) / count
    var = total(mask * adv * adv) / count - mean * mean
    white = mask * (adv - mean) * lax.rsqrt(var + WHITEN_EPS)
    for out, z in ((v_ref, values), (ret_ref, mask * (adv + values)), (white_ref, white)):
        mine = z[:ROWS]
        moved = mine
        for piece in range(1, CP):
            moved = jnp.where(cp == piece, pltpu.roll(mine, SEQ - piece * PIECE, 1), moved)
        out[...] = moved[:, :PIECE]


def vmem():
    return pl.BlockSpec(memory_space=pltpu.VMEM)


def smem():
    return pl.BlockSpec(memory_space=pltpu.SMEM)


def hbm():
    return pl.BlockSpec(memory_space=pl.ANY)


def solution(mesh):
    def local_step(x_blk, norm_gain, w_gate, w_up, w_down, final_gain, w_value, b_value, rew_blk, mask_blk):
        rows, piece, model = x_blk.shape
        f32, bf16 = jnp.float32, jnp.bfloat16
        x = x_blk.reshape(TOK, model)
        width = model // SEND_CHUNKS
        slot_shapes = tuple(jax.ShapeDtypeStruct((SLOTS,) + z, bf16) for z in ((model, FC), (model, FC), (FC, model)))
        vec = jax.ShapeDtypeStruct((1, model), f32)
        xs, code, cnt, gm, gain, final, wv, *slots = pl.pallas_call(
            gather_kernel,
            name='gather_tokens',
            out_shape=(jax.ShapeDtypeStruct((TOK, model), bf16), jax.ShapeDtypeStruct((TOK, SEQ), f32),
                       jax.ShapeDtypeStruct((8, 128), f32), jax.ShapeDtypeStruct((2, DP * ROWS, SEQ), f32), vec, vec, vec) + slot_shapes,
            in_specs=[hbm()] * 9,
            out_specs=(vmem(),) * 10,
            scratch_shapes=[
                pltpu.VMEM((TOK, model), bf16),
                pltpu.VMEM((rows, piece), jnp.int32), pltpu.VMEM((rows, piece), f32),
                pltpu.VMEM((SEND_CHUNKS, WINDOW, width), f32), pltpu.VMEM((SEND_CHUNKS, WINDOW, width), f32),
                pltpu.VMEM((2, ROWS, SEQ), f32), pltpu.VMEM((DP * CP - 1, 2, ROWS, SEQ), f32),
                pltpu.VMEM((2, ROWS, SEQ), f32), pltpu.VMEM((2, ROWS, SEQ), f32),
                pltpu.SemaphoreType.DMA((3, SLOTS)), pltpu.SemaphoreType.DMA((6,)),
                pltpu.SemaphoreType.DMA((DP * CP - 1,)), pltpu.SemaphoreType.DMA((DP * CP - 1,)),
                pltpu.SemaphoreType.DMA, pltpu.SemaphoreType.DMA,
                pltpu.SemaphoreType.DMA((SEND_CHUNKS,)), pltpu.SemaphoreType.DMA((SEND_CHUNKS,)),
            ],
            compiler_params=pltpu.CompilerParams(collective_id=0, has_side_effects=True, vmem_limit_bytes=11 << 20),
        )(*(pltpu.with_memory_space_constraint(z, pltpu.HBM) for z in (x, mask_blk, rew_blk, norm_gain.reshape(1, model), final_gain.reshape(1, model),
                      w_value.reshape(1, model), w_gate, w_up, w_down)))
        vals, *_ = pl.pallas_call(
            mlp_kernel,
            name='active_mlp',
            out_shape=(jax.ShapeDtypeStruct((ROWS, SEQ), f32),) + slot_shapes,
            in_specs=[vmem()] * 6 + [smem()] + [hbm()] * 3 + [vmem()] * 3,
            out_specs=(vmem(),) * 4,
            input_output_aliases={10: 1, 11: 2, 12: 3},
            scratch_shapes=[
                pltpu.VMEM((TOK, model), bf16), pltpu.VMEM((TOK, model), f32), pltpu.VMEM((SIZES[-1], UNIT * FC), bf16),
                pltpu.SemaphoreType.DMA((3, SLOTS)),
            ],
            compiler_params=pltpu.CompilerParams(vmem_limit_bytes=12 << 20),
        )(cnt, xs, code, gain, final, wv, b_value.reshape(1),
          *(pltpu.with_memory_space_constraint(z, pltpu.HBM) for z in (w_gate, w_up, w_down)), *slots)
        both = pl.pallas_call(
            share_kernel,
            name='share_values',
            out_shape=jax.ShapeDtypeStruct((DP * ROWS, SEQ), f32),
            in_specs=[vmem()],
            out_specs=vmem(),
            scratch_shapes=[
                pltpu.VMEM((DP * CP - 1, ROWS, SEQ), f32),
                pltpu.SemaphoreType.DMA((DP * CP - 1,)), pltpu.SemaphoreType.DMA((DP * CP - 1,)),
            ],
            compiler_params=pltpu.CompilerParams(collective_id=1, has_side_effects=True, vmem_limit_bytes=4 << 20),
        )(vals)
        block = jax.ShapeDtypeStruct((rows, piece), f32)
        return pl.pallas_call(
            gae_kernel,
            name='gae',
            out_shape=(block, block, block),
            in_specs=[vmem(), vmem()],
            out_specs=(vmem(),) * 3,
            compiler_params=pltpu.CompilerParams(vmem_limit_bytes=4 << 20),
        )(both, gm)

    tok_spec = P('dp', 'cp')
    in_specs = (P('dp', 'cp', None), P(None), P(None, None), P(None, None), P(None, None), P(None), P(None), P(),
                tok_spec, tok_spec)
    return jax.shard_map(local_step, mesh=mesh, in_specs=in_specs, out_specs=(tok_spec,) * 3, check_vma=False)
```
